8 devices in a mesh: batch: 1 (over z), col: 2 (over y), row: 4 (over x, core).
Axes of the slice: x: 2, y: 2, z: 1, core: 2. Of those that a mesh axis runs over, the one named last changes fastest.
Arguments:
- x: bfloat16 [16, 32, 512, 32], P('batch', 'row', 'col')
- w_down_1: bfloat16 [3, 3, 32, 64], replicated
- b_down_1: float32 [64], replicated
- w_conv_1: bfloat16 [3, 3, 64, 64], replicated
- b_conv_1: float32 [64], replicated
- w_proj_1: bfloat16 [32, 64], replicated
- w_down_2: bfloat16 [3, 3, 64, 128], replicated
- b_down_2: float32 [128], replicated
- w_conv_2: bfloat16 [3, 3, 128, 128], replicated
- b_conv_2: float32 [128], replicated
- w_proj_2: bfloat16 [64, 128], replicated
- w_down_3: bfloat16 [3, 3, 128, 256], replicated
- b_down_3: float32 [256], replicated
- w_conv_3: bfloat16 [3, 3, 256, 256], replicated
- b_conv_3: float32 [256], replicated
- w_proj_3: bfloat16 [128, 256], replicated
Outputs:
- output: bfloat16 [16, 4, 64, 256], P('batch', 'row', 'col')
All inputs are finite; a program needn't handle non-finite values.
Results may differ from the reference program's by a relative error of at most 0.00239.
Values are sent between devices in bfloat16 or wider.
A program may use at most 1 GiB of HBM per device.

```python
import jax
import jax.numpy as jnp
from jax import lax

IMAGES = 16
TILE_H = 8
TILE_W = 256
ROW_DEVS = 4
COL_DEVS = 2
CHAN_0 = 32
CHAN_1 = 64
CHAN_2 = 128
CHAN_3 = 256
HEIGHT = TILE_H * ROW_DEVS
WIDTH = TILE_W * COL_DEVS
CONV_DIMS = ("NHWC", "HWIO", "NHWC")


def setup_inputs(seed: int = 0, part: int = 0) -> dict:
    root_key = jax.random.key(seed)
    image_key = jax.random.fold_in(jax.random.fold_in(root_key, 1), part)
    inputs = {"x": jax.random.normal(image_key, (IMAGES, HEIGHT, WIDTH, CHAN_0), jnp.float32).astype(jnp.bfloat16)}
    widths = (CHAN_0, CHAN_1, CHAN_2, CHAN_3)
    for stage in range(3):
        c_in = widths[stage]
        c_out = widths[stage + 1]
        stage_keys = jax.random.split(jax.random.fold_in(root_key, 10 + stage), 5)
        suffix = str(stage + 1)
        inputs["w_down_" + suffix] = (jax.random.normal(stage_keys[0], (3, 3, c_in, c_out), jnp.float32) * (9 * c_in) ** -0.5).astype(jnp.bfloat16)
        inputs["b_down_" + suffix] = 0.5 * jax.random.normal(stage_keys[1], (c_out,), jnp.float32)
        inputs["w_conv_" + suffix] = (jax.random.normal(stage_keys[2], (3, 3, c_out, c_out), jnp.float32) * (9 * c_out) ** -0.5).astype(jnp.bfloat16)
        inputs["b_conv_" + suffix] = 0.5 * jax.random.normal(stage_keys[3], (c_out,), jnp.float32)
        inputs["w_proj_" + suffix] = (jax.random.normal(stage_keys[4], (c_in, c_out), jnp.float32) * c_in ** -0.5).astype(jnp.bfloat16)
    return inputs


def conv_same(act_in, weight, stride):
    return lax.conv_general_dilated(act_in.astype(jnp.float32), weight.astype(jnp.float32), (stride, stride), ((1, 1), (1, 1)), dimension_numbers=CONV_DIMS)


def basic_block(z_prev, w_down, b_down, w_conv, b_conv, w_proj):
    y_act = jax.nn.relu(conv_same(z_prev, w_down, 2) + b_down).astype(jnp.bfloat16)
    shortcut = jnp.einsum("bhwc,cd->bhwd", z_prev[:, ::2, ::2].astype(jnp.float32), w_proj.astype(jnp.float32))
    return jax.nn.relu(conv_same(y_act, w_conv, 1) + shortcut + b_conv).astype(jnp.bfloat16)


def reference(x, w_down_1, b_down_1, w_conv_1, b_conv_1, w_proj_1, w_down_2, b_down_2, w_conv_2, b_conv_2, w_proj_2, w_down_3, b_down_3, w_conv_3, b_conv_3, w_proj_3):
    params = ((w_down_1, b_down_1, w_conv_1, b_conv_1, w_proj_1), (w_down_2, b_down_2, w_conv_2, b_conv_2, w_proj_2), (w_down_3, b_down_3, w_conv_3, b_conv_3, w_proj_3))

    def one_image(image):
        act_out = image[None]
        for stage_params in params:
            act_out = basic_block(act_out, stage_params[0], stage_params[1], stage_params[2], stage_params[3], stage_params[4])
        return act_out[0]

    return lax.map(one_image, x)
```

```python
import functools

import jax
import jax.numpy as jnp
from jax import lax
from jax.experimental import pallas as pl
from jax.experimental.pallas import tpu as pltpu
from jax.sharding import PartitionSpec as P

MESH = pl.DeviceIdType.MESH
BF = jnp.bfloat16
F32 = jnp.float32

L = 128
LL = 2 * L
H = L // 2
Q = L // 4
LO = slice(0, L)
HI = slice(L, LL)
IMG = 16
N = 5
PAD = 12
COLS = (140, 70, 35)
M = tuple(p // N for p in COLS)
MH = M[0] // 2
STEP = 132
TAPS = range(3)
MIB = 1024 * 1024

(X_TOP, X_COL, Y1_DOWN, Y1_UP, Z1_DOWN, Y2_DOWN, Y2_UP, Z2_DOWN, Y3_DOWN, Y3_UP, MESSAGES) = range(11)


def _dot(a, b):
    return jnp.dot(a, b, preferred_element_type=F32)


def _flat(v):
    return v.reshape(v.shape[0] * v.shape[1], v.shape[2])


def _roll(v, shift):
    return pltpu.roll(v, shift, v.ndim - 1)


def _lane(shape):
    return lax.broadcasted_iota(jnp.int32, shape, len(shape) - 1)


def _relu(v):
    return jnp.maximum(v, 0.0)


def _body(row_count, *refs):
    (x_hbm, wd1_h, bd1, wc1_h, bc1, wp1_h, wd2_h, bd2, wc2_h, bc2, wp2_h, wd3_h, bd3, wc3_h, bc3, wp3_h,
     out_ref,
     xv, xt, xtop, xh, fs, sdiag, rdiag, bias,
     wd1r, wc1r, wp1r, wd2r, wc2r, wp2r, wd3, wc3, wp3,
     wd1, wdh1, wc1, wch1, wpp1, wd2, wdh2, wc2, wch2, wpp2,
     part1, part2, part3, acc1, acc2, acc3, y1, y2, y3, z1, z2, zo,
     sy1d, sy1u, sz1, ry1d, ry1u, rz1,
     yh1, yh2, yt3, yb3, zh1, zh2,
     xsem, wsem, ssem, rsem) = refs

    row = lax.axis_index("row")
    col = lax.axis_index("col")
    outer, inner = col, 1 - col
    has_up = row > 0
    has_down = row < row_count - 1
    up = {"row": row - 1}
    down = {"row": row + 1}
    side = {"col": 1 - col}
    diag_down = {"row": row + 1, "col": 1 - col}
    diag_up = {"row": row - 1, "col": 1 - col}

    barrier = pltpu.get_barrier_semaphore()

    def greet(device):
        pl.semaphore_signal(barrier, inc=1, device_id=device, device_id_type=MESH)

    greet(side)

    @pl.when(has_up)
    def _():
        greet(up)
        greet(diag_up)

    @pl.when(has_down)
    def _():
        greet(down)
        greet(diag_down)

    def x_copy(h):
        return pltpu.make_async_copy(x_hbm.at[:, :, :, pl.ds(pl.multiple_of(h * L, L), L)], xv.at[h], xsem.at[h])

    w_copies = [pltpu.make_async_copy(s, d, wsem.at[i]) for i, (s, d) in enumerate(
        ((wd1_h, wd1r), (wc1_h, wc1r), (wp1_h, wp1r), (wd2_h, wd2r), (wc2_h, wc2r), (wp2_h, wp2r),
         (wd3_h, wd3), (wc3_h, wc3), (wp3_h, wp3)))]
    w_copies[0].start()
    x_copy(inner).start()
    x_copy(outer).start()
    for c in w_copies[1:]:
        c.start()

    def remote(src, dst, msg, k, dev):
        return pltpu.make_async_remote_copy(src_ref=src, dst_ref=dst, send_sem=ssem.at[msg, k], recv_sem=rsem.at[msg, k],
                                            device_id=dev, device_id_type=MESH)

    def m_xtop(h):
        return remote(x_hbm.at[:, 7, :, pl.ds(pl.multiple_of(h * L, L), L)], xtop.at[h], X_TOP, h, down)

    def m_diag():
        return remote(sdiag, rdiag, X_TOP, 2, diag_down)

    own_edge = 1 + (L - PAD) * inner + PAD * col
    far_edge = 1 + L * col

    def m_xcol():
        return remote(xt.at[pl.ds(own_edge, PAD)], xt.at[pl.ds(far_edge, PAD)], X_COL, 0, side)

    def plain(src, dst, msg, dev, first, size, src_lanes=None, dst_lanes=None):
        def make(k):
            s = pl.ds(first + order(k) * size, size)
            return remote(src.at[s] if src_lanes is None else src.at[s, :, src_lanes],
                          dst.at[s] if dst_lanes is None else dst.at[s, :, dst_lanes], msg, k, dev)
        return make

    def order(k):
        return k + col * (N - 1 - 2 * k)

    lanes_lo, lanes_hi = pl.ds(0, L), pl.ds(L, L)
    m_y1d = plain(sy1d, ry1d, Y1_DOWN, down, 0, MH)
    m_y1u = plain(sy1u, ry1u, Y1_UP, up, 0, MH)
    m_z1 = plain(sz1, rz1, Z1_DOWN, down, 0, MH)
    m_y2d = plain(y2, yh2, Y2_DOWN, down, 1, M[1], lanes_hi, lanes_lo)
    m_y2u = plain(y2, yh2, Y2_UP, up, 1, M[1], lanes_lo, lanes_hi)
    m_y3d = plain(y3, yt3, Y3_DOWN, down, 1, M[2])
    m_y3u = plain(y3, yb3, Y3_UP, up, 1, M[2])

    def m_z2(k):
        s = pl.ds(1 + order(k) * M[2], M[2])
        return remote(z2.at[s, :, :, lanes_hi], zh2.at[s], Z2_DOWN, k, down)

    def send(downs, ups, k):
        if downs:
            @pl.when(has_down)
            def _():
                for m in downs:
                    m(k).start()
        if ups:
            @pl.when(has_up)
            def _():
                for m in ups:
                    m(k).start()

    def recv(downs, ups, k):
        if downs:
            @pl.when(has_up)
            def _():
                for m in downs:
                    m(k).wait_recv()
        if ups:
            @pl.when(has_down)
            def _():
                for m in ups:
                    m(k).wait_recv()

    for ref in (xt, xh, z1, z2, zh1, zh2, y1, y2, y3, yh1, yh2, yt3, yb3):
        ref[0] = jnp.zeros(ref.shape[1:], BF)
    for ref in (y1, y2, y3, yh1, yh2, yt3, yb3):
        ref[ref.shape[0] - 1] = jnp.zeros(ref.shape[1:], BF)
    for i, (b, reps) in enumerate(((bd1, 4), (bc1, 4), (bd2, 2), (bc2, 2), (bd3, 1), (bc3, 1))):
        v = jnp.concatenate([b[...]] * reps, axis=-1)
        bias[i] = jnp.broadcast_to(v, (IMG, LL))

    neighbours = 1 + 2 * jnp.minimum(row, 1) + 2 * jnp.minimum(row_count - 1 - row, 1)
    pl.semaphore_wait(barrier, neighbours)

    send([m_xtop], [], outer)
    send([m_xtop], [], inner)

    @pl.when(jnp.logical_not(has_up))
    def _():
        for ref in (xtop, rdiag, ry1d, rz1, zh2, yt3):
            ref[...] = jnp.zeros(ref.shape, BF)
        yh2[:, :, LO] = jnp.zeros((yh2.shape[0], IMG, L), BF)

    @pl.when(jnp.logical_not(has_down))
    def _():
        for ref in (ry1u, yb3):
            ref[...] = jnp.zeros(ref.shape, BF)
        yh2[:, :, HI] = jnp.zeros((yh2.shape[0], IMG, L), BF)

    def toeplitz(dst, rows_in, rows_out, shape, piece):
        for r in range(rows_in):
            parts = []
            for i in range(rows_out):
                v = piece(r, i)
                parts.append(jnp.zeros(shape, BF) if v is None else v)
            dst[r * shape[0]:(r + 1) * shape[0], :] = jnp.concatenate(parts, axis=1)

    def tap_of(w, kw, stride):
        def piece(r, i):
            kh = r - stride * i + 1
            return w[kh, kw] if kh in TAPS else None
        return piece

    w_copies[0].wait()
    s_d1, s_c1 = wd1r.shape[2:], wc1r.shape[2:]
    for kw in TAPS:
        toeplitz(wd1.at[kw], 8, 4, s_d1, tap_of(wd1r, kw, 2))
    toeplitz(wdh1, 4, 2, s_d1, lambda r, i: wd1r[0, r] if r in TAPS and i == 0 else None)

    def transpose_half(h):
        for n in range(IMG):
            for g in range(2):
                block = xv[h, n, 4 * g:4 * g + 4].reshape(L, L)
                fs[g, n * STEP:n * STEP + L, :] = block.T.astype(F32)
        base = 1 + PAD * col + H * h

        @pl.loop(0, H, unroll=8)
        def _(p):
            for e in range(2):
                v = [fs[g, pl.ds(2 * p + e, IMG, stride=STEP), :] for g in range(2)]
                xt[base + p, e] = jnp.concatenate(v, axis=-1).astype(BF)

    def transpose_top(h):
        for n in range(IMG):
            block = jnp.concatenate([xtop[h, n]] * 4, axis=0)
            fs[0, n * STEP:n * STEP + L, :] = block.T.astype(F32)
        base = 1 + PAD * col + H * h

        @pl.loop(0, H, unroll=8)
        def _(p):
            for e in range(2):
                xh[base + p, e] = fs[0, pl.ds(2 * p + e, IMG, stride=STEP), :].astype(BF)

    quads = (PAD // 2, 4, IMG, L)

    def pack_diag():
        v = xt[pl.ds(own_edge, PAD), :, :, HI].astype(F32).reshape(quads)
        ln = _lane((quads[0], IMG, L))
        r = v[:, 3]
        for q in TAPS:
            r = jnp.where((ln >= q * Q) & (ln < (q + 1) * Q), _roll(v[:, q], (q + 1) * Q), r)
        sdiag[...] = r.astype(BF)

    def unpack_diag():
        v = rdiag[...].astype(F32)
        ln = _lane(v.shape)
        out = []
        for q in range(4):
            r = jnp.where((ln >= q * Q) & (ln < (q + 1) * Q), v, 0.0)
            r = r + _roll(r, Q)
            out.append(r + _roll(r, H))
        u = jnp.stack(out, axis=1).astype(BF)
        xh[pl.ds(1 + L * (1 - col), PAD)] = u.reshape(PAD, 2, IMG, L)

    x_copy(inner).wait()
    transpose_half(inner)
    m_xcol().start()
    pack_diag()

    @pl.when(has_down)
    def _():
        m_diag().start()

    x_copy(outer).wait()
    transpose_half(outer)

    def taps(ref, j0, m):
        return [_flat(ref[pl.ds(j0 + t, m)]) for t in TAPS]

    def pair_taps(ref, j0, m):
        return [_flat(ref[pl.ds(j0, m), 1]), _flat(ref[pl.ds(j0 + 1, m), 0]), _flat(ref[pl.ds(j0 + 1, m), 1])]

    def sum_dots(lhs, w):
        v = _dot(lhs[0], w(0))
        for t in TAPS[1:]:
            v = v + _dot(lhs[t], w(t))
        return v

    def tiles(v, m):
        return v.reshape(m, IMG, v.shape[-1])

    low = _lane((MH, IMG, L)) < H

    def pack(a, b):
        return jnp.where(low, a, b).astype(BF)

    m1, m2, m3 = M

    def down1(k):
        j0 = order(k) * m1
        v = tiles(sum_dots(pair_taps(xt, j0, m1), lambda t: wd1[t]), m1)
        part1[pl.ds(j0, m1)] = v[:, :, LO]
        hi = _relu(v[:, :, HI] + bias[0, :, HI])
        y1[pl.ds(1 + j0, m1), :, HI] = hi.astype(BF)
        sy1d[pl.ds(order(k) * MH, MH)] = pack(_roll(hi[:MH], H), hi[MH:])

    def top1(k):
        j0 = order(k) * m1
        a, b, c = pair_taps(xh, j0, m1)
        ln = _lane(a.shape)
        v = tiles(_dot(jnp.where(ln < Q, a, jnp.where(ln < H, b, c)), wdh1[...]), m1)
        lo = _relu(v + part1[pl.ds(j0, m1)] + bias[0, :, LO])
        y1[pl.ds(1 + j0, m1), :, LO] = lo.astype(BF)
        sy1u[pl.ds(order(k) * MH, MH)] = pack(lo[:MH], _roll(lo[MH:], H))

    def conv1(k):
        j0 = order(k) * m1
        v = sum_dots(taps(y1, j0, m1), lambda t: wc1[t]) + _dot(_flat(xt[pl.ds(j0 + 1, m1), 0]), wpp1[...])
        acc1[pl.ds(j0, m1)] = tiles(v, m1) + bias[1]

    def unpack1(k):
        s = pl.ds(order(k) * MH, MH)
        t, b = ry1d[s].astype(F32), ry1u[s].astype(F32)
        yh1[pl.ds(1 + order(k) * m1, MH)] = pack(t, _roll(b, H))
        yh1[pl.ds(1 + order(k) * m1 + MH, MH)] = pack(_roll(t, H), b)

    def halo1(k):
        j0 = order(k) * m1
        v = tiles(sum_dots(taps(yh1, j0, m1), lambda t: wch1[t]), m1)
        v = _relu(v + acc1[pl.ds(j0, m1)])
        z1[pl.ds(1 + order(k) * MH, MH)] = v.astype(BF).reshape(MH, 2, IMG, LL)
        hi = v[:, :, HI]
        sz1[pl.ds(order(k) * MH, MH)] = pack(_roll(hi[:MH], H), hi[MH:])

    def down2(k):
        j0 = order(k) * m2
        v = tiles(sum_dots(pair_taps(z1, j0, m2), lambda t: wd2[t]), m2)
        part2[pl.ds(j0, m2)] = v[:, :, LO]
        y2[pl.ds(1 + j0, m2), :, HI] = _relu(v[:, :, HI] + bias[2, :, HI]).astype(BF)

    def unpack2(k):
        s = order(k) * MH
        half = MH // 2
        t = rz1[pl.ds(s, MH)].astype(F32)
        u = _roll(t, H)
        zh1[pl.ds(1 + s, half)] = pack(t, u).reshape(half, 2, IMG, L)
        zh1[pl.ds(1 + s + half, half)] = pack(u, t).reshape(half, 2, IMG, L)

    def top2(k):
        j0 = order(k) * m2
        a, b, c = pair_taps(zh1, j0, m2)
        t = jnp.concatenate([jnp.where(_lane(a.shape) < H, a, b), c], axis=-1)
        v = tiles(_dot(t, wdh2[...]), m2) + part2[pl.ds(j0, m2)]
        y2[pl.ds(1 + j0, m2), :, LO] = _relu(v + bias[2, :, LO]).astype(BF)

    def conv2(k):
        j0 = order(k) * m2
        v = sum_dots(taps(y2, j0, m2), lambda t: wc2[t]) + _dot(_flat(z1[pl.ds(j0 + 1, m2), 0]), wpp2[...])
        acc2[pl.ds(j0, m2)] = tiles(v, m2) + bias[3]

    def halo2(k):
        j0 = order(k) * m2
        v = tiles(sum_dots(taps(yh2, j0, m2), lambda t: wch2[t]), m2) + acc2[pl.ds(j0, m2)]
        z2[pl.ds(1 + order(k) * m3, m3)] = _relu(v).astype(BF).reshape(m3, 2, IMG, LL)

    def down3(k):
        j0 = order(k) * m3
        v = sum_dots(pair_taps(z2, j0, m3), lambda t: wd3[1:, t].reshape(LL, LL))
        part3[pl.ds(j0, m3)] = tiles(v, m3) + bias[4]

    def top3(k):
        j0 = order(k) * m3
        v = tiles(sum_dots(pair_taps(zh2, j0, m3), lambda t: wd3[0, t]), m3) + part3[pl.ds(j0, m3)]
        y3[pl.ds(1 + j0, m3)] = _relu(v).astype(BF)

    def conv3(k):
        j0 = order(k) * m3
        v = sum_dots(taps(y3, j0, m3), lambda t: wc3[1, t]) + _dot(_flat(z2[pl.ds(j0 + 1, m3), 0, :, LO]), wp3[...])
        acc3[pl.ds(j0, m3)] = tiles(v, m3) + bias[5]

    def halo3(k):
        j0 = order(k) * m3
        v = sum_dots(taps(yt3, j0, m3), lambda t: wc3[0, t]) + sum_dots(taps(yb3, j0, m3), lambda t: wc3[2, t])
        v = _relu(tiles(v, m3) + acc3[pl.ds(j0, m3)])
        r = pl.ds(pl.multiple_of(j0 * IMG, IMG), m3 * IMG)
        zo[0, r] = _flat(v[:, :, LO])
        zo[1, r] = _flat(v[:, :, HI])

    last = N - 1

    def wait_next(downs, ups, k):
        if k == 0:
            recv(downs, ups, 0)
        if k < last:
            recv(downs, ups, k + 1)

    for k in range(N - 1):
        down1(k)
        send([m_y1d], [], k)

    recv([m_xtop], [], outer)
    transpose_top(outer)
    for k in range(2):
        top1(k)
        send([], [m_y1u], k)

    for c in w_copies[1:]:
        c.wait()
    for kw in TAPS:
        toeplitz(wc1.at[kw], 4, 4, s_c1, tap_of(wc1r, kw, 1))
    toeplitz(wpp1, 8, 4, s_d1, lambda r, i: wp1r[...] if r == 2 * i else None)

    recv([m_xtop], [], inner)
    transpose_top(inner)
    for k in range(2, N - 1):
        conv1(k - 2)
        top1(k)
        send([], [m_y1u], k)

    for kw in TAPS:
        toeplitz(wch1.at[kw], 2, 4, s_c1, lambda r, i: wc1r[2 * r, kw] if i == 3 * r else None)
    m_xcol().wait_recv()
    conv1(2)
    down1(last)
    send([m_y1d], [], last)

    @pl.when(has_up)
    def _():
        m_diag().wait_recv()

    unpack_diag()
    top1(last)
    send([], [m_y1u], last)

    s_d2, s_c2 = wd2r.shape[2:], wc2r.shape[2:]
    for kw in TAPS:
        toeplitz(wd2.at[kw], 4, 2, s_d2, tap_of(wd2r, kw, 2))
        toeplitz(wc2.at[kw], 2, 2, s_c2, tap_of(wc2r, kw, 1))
        toeplitz(wch2.at[kw], 2, 2, s_c2, lambda r, i: wc2r[2 * r, kw] if i == r else None)
    toeplitz(wpp2, 4, 2, s_d2, lambda r, i: wp2r[...] if r == 2 * i else None)
    toeplitz(wdh2, 4, 1, s_d2, lambda r, i: wd2r[0, r] if r in TAPS else None)

    conv1(3)
    recv([m_y1d], [m_y1u], 0)
    unpack1(0)
    for k in range(N):
        if k < last:
            recv([m_y1d], [m_y1u], k + 1)
            unpack1(k + 1)
        if k == 0:
            conv1(last)
        if k >= 2:
            down2(k - 2)
        halo1(k)
        send([m_z1], [], k)
        if k >= 2:
            send([m_y2d], [], k - 2)

    recv([m_z1], [], 0)
    unpack2(0)
    for k in range(N):
        if k < last:
            recv([m_z1], [], k + 1)
            unpack2(k + 1)
        if k < 2:
            down2(k + 3)
        else:
            conv2(k - 2)
        top2(k)
        send([], [m_y2u], k)
        if k < 2:
            send([m_y2d], [], k + 3)

    for k in range(N):
        wait_next([m_y2d], [m_y2u], k)
        if k < 2:
            conv2(k + 3)
        else:
            down3(k - 2)
        halo2(k)
        send([m_z2], [], k)

    for k in range(N):
        wait_next([m_z2], [], k)
        if k < 2:
            down3(k + 3)
        else:
            conv3(k - 2)
        top3(k)
        send([m_y3d], [m_y3u], k)

    for k in range(N):
        wait_next([m_y3d], [m_y3u], k)
        if k < 2:
            conv3(k + 3)
        halo3(k)

    for n in range(IMG):
        v = [zo[g, pl.ds(PAD * 4 * col + n, out_ref.shape[2], stride=IMG), :] for g in range(2)]
        out_ref[n, 0] = jnp.concatenate(v, axis=-1).astype(BF)

    m_xcol().wait_send()

    @pl.when(has_down)
    def _():
        m_diag().wait_send()
        for h in range(2):
            m_xtop(h).wait_send()

        @pl.loop(0, N)
        def _(k):
            for m in (m_y1d, m_z1, m_y2d, m_z2, m_y3d):
                m(k).wait_send()

    @pl.when(has_up)
    def _():
        @pl.loop(0, N)
        def _(k):
            for m in (m_y1u, m_y2u, m_y3u):
                m(k).wait_send()


def solution(mesh):
    row_count = mesh.shape["row"]
    tile_spec = P("batch", "row", "col")
    c1, c2, c3 = COLS

    def vm(*shape, dtype=BF):
        return pltpu.VMEM(shape, dtype)

    def weights(cin, cout):
        return [vm(3, 3, cin, cout), vm(3, 3, cout, cout), vm(cin, cout)]

    packed = vm(c2, IMG, L)
    scratch = [
        vm(2, IMG, 8, Q, L), vm(c1 + 1, 2, IMG, LL), vm(2, IMG, Q, L), vm(c1 + 1, 2, IMG, L),
        vm(2, IMG * STEP, L, dtype=F32), vm(PAD // 2, IMG, L), vm(PAD // 2, IMG, L), vm(6, IMG, LL, dtype=F32),
        *weights(Q, H), *weights(H, L), *weights(L, LL),
        vm(3, LL, LL), vm(L, L), vm(3, LL, LL), vm(3, L, LL), vm(LL, LL),
        vm(3, LL, LL), vm(LL, L), vm(3, LL, LL), vm(3, LL, LL), vm(LL, LL),
        vm(c1, IMG, L, dtype=F32), vm(c2, IMG, L, dtype=F32), vm(c3, IMG, LL, dtype=F32),
        vm(c1, IMG, LL, dtype=F32), vm(c2, IMG, LL, dtype=F32), vm(c3, IMG, LL, dtype=F32),
        vm(c1 + 2, IMG, LL), vm(c2 + 2, IMG, LL), vm(c3 + 2, IMG, LL), vm(c2 + 1, 2, IMG, LL), vm(c3 + 1, 2, IMG, LL),
        vm(2, c3 * IMG, L, dtype=F32),
        *[packed] * 6,
        vm(c1 + 2, IMG, L), vm(c2 + 2, IMG, LL), vm(c3 + 2, IMG, LL), vm(c3 + 2, IMG, LL), vm(c2 + 1, 2, IMG, L), vm(c3 + 1, 2, IMG, L),
        pltpu.SemaphoreType.DMA((2,)), pltpu.SemaphoreType.DMA((9,)),
        pltpu.SemaphoreType.DMA((MESSAGES, N)), pltpu.SemaphoreType.DMA((MESSAGES, N)),
    ]

    def local(x_tile, *params):
        x_t = jnp.transpose(x_tile, (0, 1, 3, 2))
        params = [p.reshape(1, -1) if p.ndim == 1 else p for p in params]
        specs = [pl.BlockSpec(memory_space=pltpu.HBM)]
        for p in params:
            specs.append(pl.BlockSpec(memory_space=pltpu.VMEM if p.dtype == F32 else pltpu.HBM))
        return pl.pallas_call(
            functools.partial(_body, row_count),
            out_shape=jax.ShapeDtypeStruct((IMG, 1, 32, LL), BF),
            in_specs=specs,
            out_specs=pl.BlockSpec(memory_space=pltpu.VMEM),
            scratch_shapes=scratch,
            compiler_params=pltpu.CompilerParams(collective_id=0, has_side_effects=True, vmem_limit_bytes=60 * MIB),
        )(x_t, *params)

    return jax.shard_map(local, mesh=mesh, in_specs=(tile_spec,) + (P(),) * 15, out_specs=tile_spec, check_vma=False)
```

```python
import functools

import jax
import jax.numpy as jnp
from jax import lax
from jax.experimental import pallas as pl
from jax.experimental.pallas import tpu as pltpu
from jax.sharding import PartitionSpec as P

MESH = pl.DeviceIdType.MESH
BF = jnp.bfloat16
F32 = jnp.float32

L = 128
LL = 2 * L
H = L // 2
Q = L // 4
LO = slice(0, L)
HI = slice(L, LL)
IMG = 16
N = 5
PAD = 12
NEED = (11, 7)
COLS = (140, 70, 35)
M = tuple(p // N for p in COLS)
MH = M[0] // 2
STEP = 132
TAPS = range(3)
MIB = 1024 * 1024

(X_TOP, X_COL, Y1_DOWN, Y1_UP, Z1_DOWN, Y2_DOWN, Z1_UP, Z2_DOWN, Y3_DOWN, Y3_UP, MESSAGES) = range(11)


def _dot(a, b):
    return jnp.dot(a, b, preferred_element_type=F32)


def _flat(v):
    return v.reshape(v.shape[0] * v.shape[1], v.shape[2])


def _roll(v, shift):
    return pltpu.roll(v, shift, v.ndim - 1)


def _lane(shape):
    return lax.broadcasted_iota(jnp.int32, shape, len(shape) - 1)


def _relu(v):
    return jnp.maximum(v, 0.0)


def _body(row_count, *refs):
    (x_hbm, wd1_h, bd1_h, wc1_h, bc1_h, wp1_h, wd2_h, bd2_h, wc2_h, bc2_h, wp2_h, wd3_h, bd3_h, wc3_h, bc3_h, wp3_h,
     out_ref,
     xv, xt, xtop, xh, fs, sdiag, rdiag, bias,
     wd1r, wc1r, wp1r, wd2r, wc2r, wp2r, wd3, wc3, wp3, bd1, bc1, bd2, bc2, bd3, bc3,
     wd1, wdh1, wc1, wch1, wpp1, wd2, wdh2, wdb2, wc2, wch2, wpp2,
     part1, part2, part3, acc1, acc2, acc3, y1, y2, y3, z1, z2, zo,
     sy1d, sy1u, sz1, ry1d, ry1u, rz1,
     yh1, yh2, yt3, yb3, zh1, zb1, zh2,
     xsem, wsem, ssem, rsem) = refs

    row = lax.axis_index("row")
    col = lax.axis_index("col")
    outer, inner = col, 1 - col
    has_up = row > 0
    has_down = row < row_count - 1
    up = {"row": row - 1}
    down = {"row": row + 1}
    side = {"col": 1 - col}
    diag_down = {"row": row + 1, "col": 1 - col}
    diag_up = {"row": row - 1, "col": 1 - col}

    barrier = pltpu.get_barrier_semaphore()

    def greet(device):
        pl.semaphore_signal(barrier, inc=1, device_id=device, device_id_type=MESH)

    greet(side)

    @pl.when(has_up)
    def _():
        greet(up)
        greet(diag_up)

    @pl.when(has_down)
    def _():
        greet(down)
        greet(diag_down)

    def x_copy(h):
        return pltpu.make_async_copy(x_hbm.at[:, :, :, pl.ds(pl.multiple_of(h * L, L), L)], xv.at[h], xsem.at[h])

    w_copies = [pltpu.make_async_copy(s, d, wsem.at[i]) for i, (s, d) in enumerate(
        ((wd1_h, wd1r), (bd1_h, bd1), (bc1_h, bc1), (bd2_h, bd2), (bc2_h, bc2), (bd3_h, bd3), (bc3_h, bc3),
         (wc1_h, wc1r), (wp1_h, wp1r), (wd2_h, wd2r), (wc2_h, wc2r), (wp2_h, wp2r),
         (wd3_h, wd3), (wc3_h, wc3), (wp3_h, wp3)))]
    first_copies, late_copies = w_copies[:7], w_copies[7:]
    x_copy(inner).start()
    for c in first_copies:
        c.start()
    x_copy(outer).start()

    def remote(src, dst, msg, k, dev):
        return pltpu.make_async_remote_copy(src_ref=src, dst_ref=dst, send_sem=ssem.at[msg, k], recv_sem=rsem.at[msg, k],
                                            device_id=dev, device_id_type=MESH)

    def m_xtop(h):
        return remote(xv.at[h, :, 7], xtop.at[h], X_TOP, h, down)

    def m_diag():
        return remote(sdiag, rdiag, X_TOP, 2, diag_down)

    own_edge = 1 + (L - PAD) * inner + PAD * col
    far_edge = 1 + L * col

    def m_xcol(c):
        skip = (PAD - NEED[0]) * (1 - c)
        return remote(xt.at[pl.ds(own_edge + skip, NEED[c])], xt.at[pl.ds(far_edge + skip, NEED[c])], X_COL, 0, side)

    def for_col(fn):
        for c in range(2):
            @pl.when(col == c)
            def _():
                fn(c)

    def plain(src, dst, msg, dev, first, size, src_lanes=None, dst_lanes=None):
        def make(k):
            s = pl.ds(first + order(k) * size, size)
            return remote(src.at[s] if src_lanes is None else src.at[s, :, src_lanes],
                          dst.at[s] if dst_lanes is None else dst.at[s, :, dst_lanes], msg, k, dev)
        return make

    def order(k):
        return k + col * (N - 1 - 2 * k)

    lanes_lo, lanes_hi = pl.ds(0, L), pl.ds(L, L)
    m_y1d = plain(sy1d, ry1d, Y1_DOWN, down, 0, MH)
    m_y1u = plain(sy1u, ry1u, Y1_UP, up, 0, MH)
    m_z1 = plain(sz1, rz1, Z1_DOWN, down, 0, MH)
    m_y2d = plain(y2, yh2, Y2_DOWN, down, 1, M[1], lanes_hi, lanes_lo)
    m_y3d = plain(y3, yt3, Y3_DOWN, down, 1, M[2])
    m_y3u = plain(y3, yb3, Y3_UP, up, 1, M[2])

    def m_z1u(k):
        s = pl.ds(1 + order(k) * MH, MH)
        return remote(z1.at[s, :, :, lanes_lo], zb1.at[s], Z1_UP, k, up)

    def m_z2(k):
        s = pl.ds(1 + order(k) * M[2], M[2])
        return remote(z2.at[s, :, :, lanes_hi], zh2.at[s], Z2_DOWN, k, down)

    def send(downs, ups, k):
        if downs:
            @pl.when(has_down)
            def _():
                for m in downs:
                    m(k).start()
        if ups:
            @pl.when(has_up)
            def _():
                for m in ups:
                    m(k).start()

    def recv(downs, ups, k):
        if downs:
            @pl.when(has_up)
            def _():
                for m in downs:
                    m(k).wait_recv()
        if ups:
            @pl.when(has_down)
            def _():
                for m in ups:
                    m(k).wait_recv()

    for ref in (xt, xh, z1, z2, zh1, zb1, zh2, y1, y2, y3, yh1, yh2, yt3, yb3):
        ref[0] = jnp.zeros(ref.shape[1:], BF)
    for ref in (y1, y2, y3, yh1, yh2, yt3, yb3):
        ref[ref.shape[0] - 1] = jnp.zeros(ref.shape[1:], BF)

    neighbours = 1 + 2 * jnp.minimum(row, 1) + 2 * jnp.minimum(row_count - 1 - row, 1)
    pl.semaphore_wait(barrier, neighbours)

    x_copy(outer).wait()
    x_copy(inner).wait()
    send([m_xtop], [], outer)
    send([m_xtop], [], inner)
    for c in late_copies:
        c.start()

    @pl.when(jnp.logical_not(has_up))
    def _():
        for ref in (xtop, rdiag, ry1d, rz1, zh2, yt3):
            ref[...] = jnp.zeros(ref.shape, BF)
        yh2[:, :, LO] = jnp.zeros((yh2.shape[0], IMG, L), BF)

    @pl.when(jnp.logical_not(has_down))
    def _():
        for ref in (ry1u, zb1, yb3):
            ref[...] = jnp.zeros(ref.shape, BF)

    def toeplitz(dst, rows_in, rows_out, shape, piece):
        for r in range(rows_in):
            parts = []
            for i in range(rows_out):
                v = piece(r, i)
                parts.append(jnp.zeros(shape, BF) if v is None else v)
            dst[r * shape[0]:(r + 1) * shape[0], :] = jnp.concatenate(parts, axis=1)

    def tap_of(w, kw, stride):
        def piece(r, i):
            kh = r - stride * i + 1
            return w[kh, kw] if kh in TAPS else None
        return piece

    for c in first_copies:
        c.wait()
    for i, (b, reps) in enumerate(((bd1, 4), (bc1, 4), (bd2, 2), (bc2, 2), (bd3, 1), (bc3, 1))):
        v = jnp.concatenate([b[...]] * reps, axis=-1)
        bias[i] = jnp.broadcast_to(v, (IMG, LL))
    s_d1, s_c1 = wd1r.shape[2:], wc1r.shape[2:]
    for kw in TAPS:
        toeplitz(wd1.at[kw], 8, 4, s_d1, tap_of(wd1r, kw, 2))
    toeplitz(wdh1, 4, 2, s_d1, lambda r, i: wd1r[0, r] if r in TAPS and i == 0 else None)

    def transpose_half(h):
        for n in range(IMG):
            for g in range(2):
                block = xv[h, n, 4 * g:4 * g + 4].reshape(L, L)
                fs[g, n * STEP:n * STEP + L, :] = block.T.astype(F32)

    def gather_pairs(h, lo, n):
        base = 1 + PAD * col + H * h

        @pl.loop(0, n, unroll=4)
        def _(i):
            p = lo + i
            for e in range(2):
                v = [fs[g, pl.ds(2 * p + e, IMG, stride=STEP), :] for g in range(2)]
                xt[base + p, e] = jnp.concatenate(v, axis=-1).astype(BF)

    def transpose_top(h):
        for n in range(IMG):
            block = jnp.concatenate([xtop[h, n]] * 4, axis=0)
            fs[0, n * STEP:n * STEP + L, :] = block.T.astype(F32)
        base = 1 + PAD * col + H * h

        @pl.loop(0, H, unroll=8)
        def _(p):
            for e in range(2):
                xh[base + p, e] = fs[0, pl.ds(2 * p + e, IMG, stride=STEP), :].astype(BF)

    quads = (PAD // 2, 4, IMG, L)

    def pack_diag():
        v = xt[pl.ds(own_edge, PAD), :, :, HI].astype(F32).reshape(quads)
        ln = _lane((quads[0], IMG, L))
        r = v[:, 3]
        for q in TAPS:
            r = jnp.where((ln >= q * Q) & (ln < (q + 1) * Q), _roll(v[:, q], (q + 1) * Q), r)
        sdiag[...] = r.astype(BF)

    def unpack_diag():
        v = rdiag[...].astype(F32)
        ln = _lane(v.shape)
        out = []
        for q in range(4):
            r = jnp.where((ln >= q * Q) & (ln < (q + 1) * Q), v, 0.0)
            r = r + _roll(r, Q)
            out.append(r + _roll(r, H))
        u = jnp.stack(out, axis=1).astype(BF)
        xh[pl.ds(1 + L * (1 - col), PAD)] = u.reshape(PAD, 2, IMG, L)

    border = (H - PAD) * inner
    transpose_half(inner)
    gather_pairs(inner, border, PAD)
    for_col(lambda c: m_xcol(c).start())
    pack_diag()

    @pl.when(has_down)
    def _():
        m_diag().start()

    gather_pairs(inner, PAD * col, H - PAD)
    transpose_half(outer)
    gather_pairs(outer, 0, H)

    def taps(ref, j0, m):
        return [_flat(ref[pl.ds(j0 + t, m)]) for t in TAPS]

    def pair_taps(ref, j0, m):
        return [_flat(ref[pl.ds(j0, m), 1]), _flat(ref[pl.ds(j0 + 1, m), 0]), _flat(ref[pl.ds(j0 + 1, m), 1])]

    def sum_dots(lhs, w):
        v = _dot(lhs[0], w(0))
        for t in TAPS[1:]:
            v = v + _dot(lhs[t], w(t))
        return v

    def tiles(v, m):
        return v.reshape(m, IMG, v.shape[-1])

    low = _lane((MH, IMG, L)) < H

    def pack(a, b):
        return jnp.where(low, a, b).astype(BF)

    m1, m2, m3 = M

    def down1(k):
        j0 = order(k) * m1
        v = tiles(sum_dots(pair_taps(xt, j0, m1), lambda t: wd1[t]), m1)
        part1[pl.ds(j0, m1)] = v[:, :, LO]
        hi = _relu(v[:, :, HI] + bias[0, :, HI])
        y1[pl.ds(1 + j0, m1), :, HI] = hi.astype(BF)
        sy1d[pl.ds(order(k) * MH, MH)] = pack(_roll(hi[:MH], H), hi[MH:])

    def top1(k):
        j0 = order(k) * m1
        a, b, c = pair_taps(xh, j0, m1)
        ln = _lane(a.shape)
        v = tiles(_dot(jnp.where(ln < Q, a, jnp.where(ln < H, b, c)), wdh1[...]), m1)
        lo = _relu(v + part1[pl.ds(j0, m1)] + bias[0, :, LO])
        y1[pl.ds(1 + j0, m1), :, LO] = lo.astype(BF)
        sy1u[pl.ds(order(k) * MH, MH)] = pack(lo[:MH], _roll(lo[MH:], H))

    def conv1(k):
        j0 = order(k) * m1
        v = sum_dots(taps(y1, j0, m1), lambda t: wc1[t]) + _dot(_flat(xt[pl.ds(j0 + 1, m1), 0]), wpp1[...])
        acc1[pl.ds(j0, m1)] = tiles(v, m1) + bias[1]

    def unpack1(k):
        s = pl.ds(order(k) * MH, MH)
        t, b = ry1d[s].astype(F32), ry1u[s].astype(F32)
        yh1[pl.ds(1 + order(k) * m1, MH)] = pack(t, _roll(b, H))
        yh1[pl.ds(1 + order(k) * m1 + MH, MH)] = pack(_roll(t, H), b)

    def halo1(k):
        j0 = order(k) * m1
        v = tiles(sum_dots(taps(yh1, j0, m1), lambda t: wch1[t]), m1)
        v = _relu(v + acc1[pl.ds(j0, m1)])
        z1[pl.ds(1 + order(k) * MH, MH)] = v.astype(BF).reshape(MH, 2, IMG, LL)
        hi = v[:, :, HI]
        sz1[pl.ds(order(k) * MH, MH)] = pack(_roll(hi[:MH], H), hi[MH:])

    def down2(k):
        j0 = order(k) * m2
        v = tiles(sum_dots(pair_taps(z1, j0, m2), lambda t: wd2[t]), m2)
        part2[pl.ds(j0, m2)] = v[:, :, LO]
        y2[pl.ds(1 + j0, m2), :, HI] = _relu(v[:, :, HI] + bias[2, :, HI]).astype(BF)

    def unpack2(k):
        s = order(k) * MH
        half = MH // 2
        t = rz1[pl.ds(s, MH)].astype(F32)
        u = _roll(t, H)
        zh1[pl.ds(1 + s, half)] = pack(t, u).reshape(half, 2, IMG, L)
        zh1[pl.ds(1 + s + half, half)] = pack(u, t).reshape(half, 2, IMG, L)

    def top2(k):
        j0 = order(k) * m2
        a, b, c = pair_taps(zh1, j0, m2)
        t = jnp.concatenate([jnp.where(_lane(a.shape) < H, a, b), c], axis=-1)
        v = tiles(_dot(t, wdh2[...]), m2) + part2[pl.ds(j0, m2)]
        y2[pl.ds(1 + j0, m2), :, LO] = _relu(v + bias[2, :, LO]).astype(BF)

    def bottom2(k):
        j0 = order(k) * m2
        own, below = pair_taps(z1, j0, m2), pair_taps(zb1, j0, m2)
        lhs = [jnp.concatenate([a[:, HI], b], axis=-1) for a, b in zip(own, below)]
        v = _relu(tiles(sum_dots(lhs, lambda t: wdb2[t]), m2) + bias[2, :, LO])
        yh2[pl.ds(1 + j0, m2), :, HI] = jnp.where(has_down, v, 0.0).astype(BF)

    def conv2(k):
        j0 = order(k) * m2
        v = sum_dots(taps(y2, j0, m2), lambda t: wc2[t]) + _dot(_flat(z1[pl.ds(j0 + 1, m2), 0]), wpp2[...])
        acc2[pl.ds(j0, m2)] = tiles(v, m2) + bias[3]

    def halo2(k):
        j0 = order(k) * m2
        v = tiles(sum_dots(taps(yh2, j0, m2), lambda t: wch2[t]), m2) + acc2[pl.ds(j0, m2)]
        z2[pl.ds(1 + order(k) * m3, m3)] = _relu(v).astype(BF).reshape(m3, 2, IMG, LL)

    def full2(k):
        j0 = order(k) * m2
        v = sum_dots(taps(y2, j0, m2), lambda t: wc2[t]) + _dot(_flat(z1[pl.ds(j0 + 1, m2), 0]), wpp2[...])
        v = tiles(v + sum_dots(taps(yh2, j0, m2), lambda t: wch2[t]), m2) + bias[3]
        z2[pl.ds(1 + order(k) * m3, m3)] = _relu(v).astype(BF).reshape(m3, 2, IMG, LL)

    def down3(k):
        j0 = order(k) * m3
        v = sum_dots(pair_taps(z2, j0, m3), lambda t: wd3[1:, t].reshape(LL, LL))
        part3[pl.ds(j0, m3)] = tiles(v, m3) + bias[4]

    def top3(k):
        j0 = order(k) * m3
        v = tiles(sum_dots(pair_taps(zh2, j0, m3), lambda t: wd3[0, t]), m3) + part3[pl.ds(j0, m3)]
        y3[pl.ds(1 + j0, m3)] = _relu(v).astype(BF)

    def conv3(k):
        j0 = order(k) * m3
        v = sum_dots(taps(y3, j0, m3), lambda t: wc3[1, t]) + _dot(_flat(z2[pl.ds(j0 + 1, m3), 0, :, LO]), wp3[...])
        acc3[pl.ds(j0, m3)] = tiles(v, m3) + bias[5]

    def halo3(k):
        j0 = order(k) * m3
        v = sum_dots(taps(yt3, j0, m3), lambda t: wc3[0, t]) + sum_dots(taps(yb3, j0, m3), lambda t: wc3[2, t])
        v = _relu(tiles(v, m3) + acc3[pl.ds(j0, m3)])
        r = pl.ds(pl.multiple_of(j0 * IMG, IMG), m3 * IMG)
        zo[0, r] = _flat(v[:, :, LO])
        zo[1, r] = _flat(v[:, :, HI])

    last = N - 1

    def wait_next(downs, ups, k):
        if k == 0:
            recv(downs, ups, 0)
        if k < last:
            recv(downs, ups, k + 1)

    for k in range(last):
        down1(k)
    for k in range(last):
        send([m_y1d], [], k)

    for c in late_copies:
        c.wait()
    for kw in TAPS:
        toeplitz(wc1.at[kw], 4, 4, s_c1, tap_of(wc1r, kw, 1))
        toeplitz(wch1.at[kw], 2, 4, s_c1, lambda r, i: wc1r[2 * r, kw] if i == 3 * r else None)
    toeplitz(wpp1, 8, 4, s_d1, lambda r, i: wp1r[...] if r == 2 * i else None)

    s_d2, s_c2 = wd2r.shape[2:], wc2r.shape[2:]
    for kw in TAPS:
        toeplitz(wd2.at[kw], 4, 2, s_d2, tap_of(wd2r, kw, 2))
        toeplitz(wdb2.at[kw], 4, 1, s_d2, lambda r, i: wd2r[r - 1, kw] if r else None)
        toeplitz(wc2.at[kw], 2, 2, s_c2, tap_of(wc2r, kw, 1))
        toeplitz(wch2.at[kw], 2, 2, s_c2, lambda r, i: wc2r[2 * r, kw] if i == r else None)
    toeplitz(wpp2, 4, 2, s_d2, lambda r, i: wp2r[...] if r == 2 * i else None)
    toeplitz(wdh2, 4, 1, s_d2, lambda r, i: wd2r[0, r] if r in TAPS else None)

    recv([m_xtop], [], outer)
    transpose_top(outer)
    top1(0)
    send([], [m_y1u], 0)
    top1(1)
    send([], [m_y1u], 1)

    recv([m_xtop], [], inner)
    transpose_top(inner)
    top1(2)
    top1(3)
    send([], [m_y1u], 2)
    send([], [m_y1u], 3)
    conv1(0)

    @pl.when(has_up)
    def _():
        m_diag().wait_recv()

    unpack_diag()
    for_col(lambda c: m_xcol(1 - c).wait_recv())
    down1(last)
    top1(last)
    send([m_y1d], [m_y1u], last)

    recv([m_y1d], [m_y1u], 0)
    unpack1(0)
    for k in range(N):
        if k < last:
            recv([m_y1d], [m_y1u], k + 1)
            unpack1(k + 1)
        if k >= 2:
            down2(k - 2)
        halo1(k)
        if k < last:
            conv1(k + 1)
        send([m_z1], [m_z1u], k)
        if k >= 2:
            send([m_y2d], [], k - 2)
    down2(3)
    down2(last)
    send([m_y2d], [], 3)
    send([m_y2d], [], last)

    recv([m_z1], [m_z1u], 0)
    unpack2(0)
    for k in range(3):
        recv([m_z1], [m_z1u], k + 1)
        unpack2(k + 1)
        top2(k)
        bottom2(k)
        if k:
            wait_next([m_y2d], [], k - 1)
            full2(k - 1)
            send([m_z2], [], k - 1)
    recv([m_z1], [m_z1u], last)
    unpack2(last)
    top2(3)
    bottom2(3)
    top2(last)
    bottom2(last)
    recv([m_y2d], [], 3)
    full2(2)
    send([m_z2], [], 2)
    recv([m_y2d], [], last)
    full2(3)
    full2(last)
    send([m_z2], [], 3)
    send([m_z2], [], last)

    for k in range(N):
        down3(k)
    for k in range(N):
        wait_next([m_z2], [], k)
        if k >= 2:
            conv3(k - 2)
        top3(k)
        send([m_y3d], [m_y3u], k)
    conv3(3)
    conv3(last)
    for k in range(3):
        wait_next([m_y3d], [m_y3u], k)
    for k in range(3):
        halo3(k)
    wait_next([m_y3d], [m_y3u], 3)
    halo3(3)
    halo3(last)

    for n in range(IMG):
        v = [zo[g, pl.ds(PAD * 4 * col + n, out_ref.shape[2], stride=IMG), :] for g in range(2)]
        out_ref[n, 0] = jnp.concatenate(v, axis=-1).astype(BF)

    for_col(lambda c: m_xcol(c).wait_send())

    @pl.when(has_down)
    def _():
        m_diag().wait_send()
        for h in range(2):
            m_xtop(h).wait_send()

        @pl.loop(0, N)
        def _(k):
            for m in (m_y1d, m_z1, m_y2d, m_z2, m_y3d):
                m(k).wait_send()

    @pl.when(has_up)
    def _():
        @pl.loop(0, N)
        def _(k):
            for m in (m_y1u, m_z1u, m_y3u):
                m(k).wait_send()


def solution(mesh):
    row_count = mesh.shape["row"]
    tile_spec = P("batch", "row", "col")
    c1, c2, c3 = COLS

    def vm(*shape, dtype=BF):
        return pltpu.VMEM(shape, dtype)

    def weights(cin, cout):
        return [vm(3, 3, cin, cout), vm(3, 3, cout, cout), vm(cin, cout)]

    packed = vm(c2, IMG, L)
    scratch = [
        vm(2, IMG, 8, Q, L), vm(c1 + 1, 2, IMG, LL), vm(2, IMG, Q, L), vm(c1 + 1, 2, IMG, L),
        vm(2, IMG * STEP, L, dtype=F32), vm(PAD // 2, IMG, L), vm(PAD // 2, IMG, L), vm(6, IMG, LL, dtype=F32),
        *weights(Q, H), *weights(H, L), *weights(L, LL),
        *[vm(1, c, dtype=F32) for c in (H, H, L, L, LL, LL)],
        vm(3, LL, LL), vm(L, L), vm(3, LL, LL), vm(3, L, LL), vm(LL, LL),
        vm(3, LL, LL), vm(LL, L), vm(3, LL, L), vm(3, LL, LL), vm(3, LL, LL), vm(LL, LL),
        vm(c1, IMG, L, dtype=F32), vm(c2, IMG, L, dtype=F32), vm(c3, IMG, LL, dtype=F32),
        vm(c1, IMG, LL, dtype=F32), vm(c2, IMG, LL, dtype=F32), vm(c3, IMG, LL, dtype=F32),
        vm(c1 + 2, IMG, LL), vm(c2 + 2, IMG, LL), vm(c3 + 2, IMG, LL), vm(c2 + 1, 2, IMG, LL), vm(c3 + 1, 2, IMG, LL),
        vm(2, c3 * IMG, L, dtype=F32),
        *[packed] * 6,
        vm(c1 + 2, IMG, L), vm(c2 + 2, IMG, LL), vm(c3 + 2, IMG, LL), vm(c3 + 2, IMG, LL), vm(c2 + 1, 2, IMG, L), vm(c2 + 1, 2, IMG, L), vm(c3 + 1, 2, IMG, L),
        pltpu.SemaphoreType.DMA((2,)), pltpu.SemaphoreType.DMA((15,)),
        pltpu.SemaphoreType.DMA((MESSAGES, N)), pltpu.SemaphoreType.DMA((MESSAGES, N)),
    ]

    def local(x_tile, *params):
        x_t = jnp.transpose(x_tile, (0, 1, 3, 2))
        params = [p.reshape(1, -1) if p.ndim == 1 else p for p in params]
        operands = [pltpu.with_memory_space_constraint(p, pltpu.HBM) for p in (x_t, *params)]
        return pl.pallas_call(
            functools.partial(_body, row_count),
            out_shape=pltpu.VMEM((IMG, 1, 32, LL), BF),
            in_specs=[pl.BlockSpec(memory_space=pltpu.HBM)] * len(operands),
            out_specs=pl.BlockSpec(memory_space=pltpu.VMEM),
            scratch_shapes=scratch,
            compiler_params=pltpu.CompilerParams(collective_id=0, has_side_effects=True, vmem_limit_bytes=60 * MIB),
        )(*operands)

    return jax.shard_map(local, mesh=mesh, in_specs=(tile_spec,) + (P(),) * 15, out_specs=tile_spec, check_vma=False)
```

```python
import functools

import jax
import jax.numpy as jnp
from jax import lax
from jax.experimental import pallas as pl
from jax.experimental.pallas import tpu as pltpu
from jax.sharding import PartitionSpec as P

MESH = pl.DeviceIdType.MESH
BF = jnp.bfloat16
F32 = jnp.float32

L = 128
LL = 2 * L
H = L // 2
Q = L // 4
LO = slice(0, L)
HI = slice(L, LL)
IMG = 16
N = 5
PAD = 12
NEED = (11, 7)
COLS = (140, 70, 35)
M = tuple(p // N for p in COLS)
MH = M[0] // 2
STEP = 132
TAPS = range(3)
MIB = 1024 * 1024

(X_TOP, X_COL, Y1_DOWN, Y1_UP, Z1_DOWN, Y2_DOWN, Z1_UP, Z2_DOWN, Y3_DOWN, Y3_UP, MESSAGES) = range(11)


def _dot(a, b):
    return jnp.dot(a, b, preferred_element_type=F32)


def _flat(v):
    return v.reshape(v.shape[0] * v.shape[1], v.shape[2])


def _roll(v, shift):
    return pltpu.roll(v, shift, v.ndim - 1)


def _lane(shape):
    return lax.broadcasted_iota(jnp.int32, shape, len(shape) - 1)


def _relu(v):
    return jnp.maximum(v, 0.0)


def _body(row_count, *refs):
    (x_hbm, wd1_h, bd1_h, wc1_h, bc1_h, wp1_h, wd2_h, bd2_h, wc2_h, bc2_h, wp2_h, wd3_h, bd3_h, wc3_h, bc3_h, wp3_h,
     out_ref,
     xv, xt, xtop, xh, fs, sdiag, rdiag, bias,
     wd1r, wc1r, wp1r, wd2r, wc2r, wp2r, wd3, wc3, wp3, bd1, bc1, bd2, bc2, bd3, bc3,
     wd1, wdh1, wc1, wch1, wpp1, wd2, wdh2, wdb2, wc2, wch2, wpp2,
     part1, part2, part3, acc1, acc2, acc3, y1, y2, y3, z1, z2, zo,
     sy1d, sy1u, sz1, ry1d, ry1u, rz1,
     yh1, yh2, yt3, yb3, zh1, zb1, zh2,
     xsem, wsem, ssem, rsem, near_sem) = refs

    row = lax.axis_index("row")
    col = lax.axis_index("col")
    outer, inner = col, 1 - col
    has_up = row > 0
    has_down = row < row_count - 1
    up = {"row": row - 1}
    down = {"row": row + 1}
    side = {"col": 1 - col}
    diag_down = {"row": row + 1, "col": 1 - col}

    barrier = pltpu.get_barrier_semaphore()

    def greet(device):
        pl.semaphore_signal(barrier, inc=1, device_id=device, device_id_type=MESH)

    greet(side)

    @pl.when(has_up)
    def _():
        greet(up)

    @pl.when(has_down)
    def _():
        greet(down)

    def x_copy(h):
        return pltpu.make_async_copy(x_hbm.at[:, :, :, pl.ds(pl.multiple_of(h * L, L), L)], xv.at[h], xsem.at[h])

    w_copies = [pltpu.make_async_copy(s, d, wsem.at[i]) for i, (s, d) in enumerate(
        ((wd1_h, wd1r), (bd1_h, bd1), (bc1_h, bc1), (bd2_h, bd2), (bc2_h, bc2), (bd3_h, bd3), (bc3_h, bc3),
         (wc1_h, wc1r), (wp1_h, wp1r), (wd2_h, wd2r), (wc2_h, wc2r), (wp2_h, wp2r),
         (wd3_h, wd3), (wc3_h, wc3), (wp3_h, wp3)))]
    first_copies, late_copies = w_copies[:7], w_copies[7:]
    x_copy(inner).start()
    for c in first_copies:
        c.start()
    x_copy(outer).start()

    def remote(src, dst, msg, k, dev):
        return pltpu.make_async_remote_copy(src_ref=src, dst_ref=dst, send_sem=ssem.at[msg, k], recv_sem=rsem.at[msg, k],
                                            device_id=dev, device_id_type=MESH)

    def m_xtop(h):
        return remote(xv.at[h, :, 7], xtop.at[h], X_TOP, h, down)

    def m_diag():
        return remote(sdiag, rdiag, X_TOP, 2, diag_down)

    own_edge = 1 + (L - PAD) * inner + PAD * col
    far_edge = 1 + L * col

    def m_xcol(c):
        skip = (PAD - NEED[0]) * (1 - c)
        return remote(xt.at[pl.ds(own_edge + skip, NEED[c])], xt.at[pl.ds(far_edge + skip, NEED[c])], X_COL, 0, side)

    def for_col(fn):
        for c in range(2):
            @pl.when(col == c)
            def _():
                fn(c)

    def chunk(k, size, need):
        if k == N - 1:
            return pl.ds(1 + order(k) * size + (size - need) * col, need)
        return pl.ds(1 + order(k) * size, size)

    def plain(src, dst, msg, dev, size, need, src_lanes=None, dst_lanes=None):
        def make(k):
            s = chunk(k, size, need)
            return remote(src.at[s] if src_lanes is None else src.at[s, :, src_lanes],
                          dst.at[s] if dst_lanes is None else dst.at[s, :, dst_lanes], msg, k, dev)
        return make

    def order(k):
        return k + col * (N - 1 - 2 * k)

    lanes_lo, lanes_hi = pl.ds(0, L), pl.ds(L, L)
    def packed(src, dst, msg, dev):
        def make(k):
            s = pl.ds(order(k) * MH, MH)
            return remote(src.at[s], dst.at[s], msg, k, dev)
        return make

    m_y1d = packed(sy1d, ry1d, Y1_DOWN, down)
    m_y1u = packed(sy1u, ry1u, Y1_UP, up)
    m_z1 = packed(sz1, rz1, Z1_DOWN, down)
    m_y2d = plain(y2, yh2, Y2_DOWN, down, M[1], 12, lanes_hi, lanes_lo)
    m_y3d = plain(y3, yt3, Y3_DOWN, down, M[2], 5)
    m_y3u = plain(y3, yb3, Y3_UP, up, M[2], 5)

    def m_z1u(k):
        s = chunk(k, MH, 13)
        return remote(z1.at[s, :, :, lanes_lo], zb1.at[s], Z1_UP, k, up)

    def m_z2(k):
        s = chunk(k, M[2], 6)
        return remote(z2.at[s, :, :, lanes_hi], zh2.at[s], Z2_DOWN, k, down)

    def send(downs, ups, k):
        if downs:
            @pl.when(has_down)
            def _():
                for m in downs:
                    m(k).start()
        if ups:
            @pl.when(has_up)
            def _():
                for m in ups:
                    m(k).start()

    def recv(downs, ups, k):
        if downs:
            @pl.when(has_up)
            def _():
                for m in downs:
                    m(k).wait_recv()
        if ups:
            @pl.when(has_down)
            def _():
                for m in ups:
                    m(k).wait_recv()

    for ref in (xt, xh, z1, z2, zh1, zb1, zh2, y1, y2, y3, yh1, yh2, yt3, yb3):
        ref[0] = jnp.zeros(ref.shape[1:], BF)
    for ref in (y1, y2, y3, yh1, yh2, yt3, yb3):
        ref[ref.shape[0] - 1] = jnp.zeros(ref.shape[1:], BF)

    vertical = jnp.minimum(row, 1) + jnp.minimum(row_count - 1 - row, 1)
    pl.semaphore_wait(barrier, 1 + vertical)

    x_copy(outer).wait()
    x_copy(inner).wait()
    send([m_xtop], [], outer)
    send([m_xtop], [], inner)
    @pl.when(has_up)
    def _():
        pl.semaphore_signal(near_sem, inc=1, device_id=up, device_id_type=MESH)

    @pl.when(has_down)
    def _():
        pl.semaphore_signal(near_sem, inc=1, device_id=down, device_id_type=MESH)

    for c in late_copies:
        c.start()

    @pl.when(jnp.logical_not(has_up))
    def _():
        for ref in (xtop, rdiag, ry1d, rz1, zh2, yt3):
            ref[...] = jnp.zeros(ref.shape, BF)
        yh2[:, :, LO] = jnp.zeros((yh2.shape[0], IMG, L), BF)

    @pl.when(jnp.logical_not(has_down))
    def _():
        for ref in (ry1u, zb1, yb3):
            ref[...] = jnp.zeros(ref.shape, BF)

    def toeplitz(dst, rows_in, rows_out, shape, piece):
        for r in range(rows_in):
            parts = []
            for i in range(rows_out):
                v = piece(r, i)
                parts.append(jnp.zeros(shape, BF) if v is None else v)
            dst[r * shape[0]:(r + 1) * shape[0], :] = jnp.concatenate(parts, axis=1)

    def tap_of(w, kw, stride):
        def piece(r, i):
            kh = r - stride * i + 1
            return w[kh, kw] if kh in TAPS else None
        return piece

    for c in first_copies:
        c.wait()
    for i, (b, reps) in enumerate(((bd1, 4), (bc1, 4), (bd2, 2), (bc2, 2), (bd3, 1), (bc3, 1))):
        v = jnp.concatenate([b[...]] * reps, axis=-1)
        bias[i] = jnp.broadcast_to(v, (IMG, LL))
    s_d1, s_c1 = wd1r.shape[2:], wc1r.shape[2:]
    for kw in TAPS:
        toeplitz(wd1.at[kw], 8, 4, s_d1, tap_of(wd1r, kw, 2))
    toeplitz(wdh1, 4, 2, s_d1, lambda r, i: wd1r[0, r] if r in TAPS and i == 0 else None)

    def transpose_half(h):
        for n in range(IMG):
            for g in range(2):
                block = xv[h, n, 4 * g:4 * g + 4].reshape(L, L)
                fs[g, n * STEP:n * STEP + L, :] = block.T.astype(F32)

    def gather_pairs(h, lo, n):
        base = 1 + PAD * col + H * h

        @pl.loop(0, n, unroll=4)
        def _(i):
            p = lo + i
            for e in range(2):
                v = [fs[g, pl.ds(2 * p + e, IMG, stride=STEP), :] for g in range(2)]
                xt[base + p, e] = jnp.concatenate(v, axis=-1).astype(BF)

    def transpose_top(h):
        for n in range(IMG):
            block = jnp.concatenate([xtop[h, n]] * 4, axis=0)
            fs[0, n * STEP:n * STEP + L, :] = block.T.astype(F32)
        base = 1 + PAD * col + H * h

        @pl.loop(0, H, unroll=8)
        def _(p):
            for e in range(2):
                xh[base + p, e] = fs[0, pl.ds(2 * p + e, IMG, stride=STEP), :].astype(BF)

    quads = (PAD // 2, 4, IMG, L)

    def pack_diag():
        v = xt[pl.ds(own_edge, PAD), :, :, HI].astype(F32).reshape(quads)
        ln = _lane((quads[0], IMG, L))
        r = v[:, 3]
        for q in TAPS:
            r = jnp.where((ln >= q * Q) & (ln < (q + 1) * Q), _roll(v[:, q], (q + 1) * Q), r)
        sdiag[...] = r.astype(BF)

    def unpack_diag():
        v = rdiag[...].astype(F32)
        ln = _lane(v.shape)
        out = []
        for q in range(4):
            r = jnp.where((ln >= q * Q) & (ln < (q + 1) * Q), v, 0.0)
            r = r + _roll(r, Q)
            out.append(r + _roll(r, H))
        u = jnp.stack(out, axis=1).astype(BF)
        xh[pl.ds(1 + L * (1 - col), PAD)] = u.reshape(PAD, 2, IMG, L)

    border = (H - PAD) * inner
    transpose_half(inner)
    gather_pairs(inner, border, PAD)
    for_col(lambda c: m_xcol(c).start())
    pack_diag()
    gather_pairs(inner, PAD * col, H - PAD)
    transpose_half(outer)
    gather_pairs(outer, 0, H)
    pl.semaphore_wait(near_sem, vertical)

    @pl.when(has_down)
    def _():
        m_diag().start()

    def taps(ref, j0, m):
        return [_flat(ref[pl.ds(j0 + t, m)]) for t in TAPS]

    def pair_taps(ref, j0, m):
        return [_flat(ref[pl.ds(j0, m), 1]), _flat(ref[pl.ds(j0 + 1, m), 0]), _flat(ref[pl.ds(j0 + 1, m), 1])]

    def sum_dots(lhs, w):
        v = _dot(lhs[0], w(0))
        for t in TAPS[1:]:
            v = v + _dot(lhs[t], w(t))
        return v

    def sum_narrow(lhs, w):
        pair = jnp.concatenate([w(0), w(1)], axis=0)
        return _dot(jnp.concatenate(lhs[:2], axis=-1), pair) + _dot(lhs[2], w(2))

    def tiles(v, m):
        return v.reshape(m, IMG, v.shape[-1])

    low = _lane((MH, IMG, L)) < H

    def pack(a, b):
        return jnp.where(low, a, b).astype(BF)

    m1, m2, m3 = M

    def above1(j0):
        a, b, c = pair_taps(xh, j0, m1)
        ln = _lane(a.shape)
        return tiles(_dot(jnp.where(ln < Q, a, jnp.where(ln < H, b, c)), wdh1[...]), m1)

    def store_top1(k, v):
        lo = _relu(v + bias[0, :, LO])
        y1[pl.ds(1 + order(k) * m1, m1), :, LO] = lo.astype(BF)
        sy1u[pl.ds(order(k) * MH, MH)] = pack(lo[:MH], _roll(lo[MH:], H))

    def down1(k, whole=False):
        j0 = order(k) * m1
        v = tiles(sum_dots(pair_taps(xt, j0, m1), lambda t: wd1[t]), m1)
        if whole:
            store_top1(k, v[:, :, LO] + above1(j0))
        else:
            part1[pl.ds(j0, m1)] = v[:, :, LO]
        hi = _relu(v[:, :, HI] + bias[0, :, HI])
        y1[pl.ds(1 + j0, m1), :, HI] = hi.astype(BF)
        sy1d[pl.ds(order(k) * MH, MH)] = pack(_roll(hi[:MH], H), hi[MH:])

    def top1(k):
        j0 = order(k) * m1
        store_top1(k, above1(j0) + part1[pl.ds(j0, m1)])

    def conv1(k):
        j0 = order(k) * m1
        v = sum_dots(taps(y1, j0, m1), lambda t: wc1[t]) + _dot(_flat(xt[pl.ds(j0 + 1, m1), 0]), wpp1[...])
        acc1[pl.ds(j0, m1)] = tiles(v, m1) + bias[1]

    def unpack1(k):
        s = pl.ds(order(k) * MH, MH)
        t, b = ry1d[s].astype(F32), ry1u[s].astype(F32)
        yh1[pl.ds(1 + order(k) * m1, MH)] = pack(t, _roll(b, H))
        yh1[pl.ds(1 + order(k) * m1 + MH, MH)] = pack(_roll(t, H), b)

    def halo1(k):
        j0 = order(k) * m1
        v = tiles(sum_narrow(taps(yh1, j0, m1), lambda t: wch1[t]), m1)
        v = _relu(v + acc1[pl.ds(j0, m1)])
        z1[pl.ds(1 + order(k) * MH, MH)] = v.astype(BF).reshape(MH, 2, IMG, LL)
        hi = v[:, :, HI]
        sz1[pl.ds(order(k) * MH, MH)] = pack(_roll(hi[:MH], H), hi[MH:])

    def down2(k):
        j0 = order(k) * m2
        v = tiles(sum_dots(pair_taps(z1, j0, m2), lambda t: wd2[t]), m2)
        part2[pl.ds(j0, m2)] = v[:, :, LO]
        y2[pl.ds(1 + j0, m2), :, HI] = _relu(v[:, :, HI] + bias[2, :, HI]).astype(BF)

    def unpack2(k):
        s = order(k) * MH
        half = MH // 2
        t = rz1[pl.ds(s, MH)].astype(F32)
        u = _roll(t, H)
        zh1[pl.ds(1 + s, half)] = pack(t, u).reshape(half, 2, IMG, L)
        zh1[pl.ds(1 + s + half, half)] = pack(u, t).reshape(half, 2, IMG, L)

    def top2(k):
        j0 = order(k) * m2
        a, b, c = pair_taps(zh1, j0, m2)
        t = jnp.concatenate([jnp.where(_lane(a.shape) < H, a, b), c], axis=-1)
        v = tiles(_dot(t, wdh2[...]), m2) + part2[pl.ds(j0, m2)]
        y2[pl.ds(1 + j0, m2), :, LO] = _relu(v + bias[2, :, LO]).astype(BF)

    def bottom2(k):
        j0 = order(k) * m2
        own, below = pair_taps(z1, j0, m2), pair_taps(zb1, j0, m2)
        lhs = [jnp.concatenate([a[:, HI], b], axis=-1) for a, b in zip(own, below)]
        v = _relu(tiles(sum_dots(lhs, lambda t: wdb2[t]), m2) + bias[2, :, LO])
        yh2[pl.ds(1 + j0, m2), :, HI] = jnp.where(has_down, v, 0.0).astype(BF)

    def conv2(k):
        j0 = order(k) * m2
        v = sum_dots(taps(y2, j0, m2), lambda t: wc2[t]) + _dot(_flat(z1[pl.ds(j0 + 1, m2), 0]), wpp2[...])
        acc2[pl.ds(j0, m2)] = tiles(v, m2) + bias[3]

    def halo2(k):
        j0 = order(k) * m2
        v = tiles(sum_dots(taps(yh2, j0, m2), lambda t: wch2[t]), m2) + acc2[pl.ds(j0, m2)]
        z2[pl.ds(1 + order(k) * m3, m3)] = _relu(v).astype(BF).reshape(m3, 2, IMG, LL)

    def down3(k):
        j0 = order(k) * m3
        v = sum_dots(pair_taps(z2, j0, m3), lambda t: wd3[1:, t].reshape(LL, LL))
        part3[pl.ds(j0, m3)] = tiles(v, m3) + bias[4]

    def top3(k):
        j0 = order(k) * m3
        v = tiles(sum_narrow(pair_taps(zh2, j0, m3), lambda t: wd3[0, t]), m3) + part3[pl.ds(j0, m3)]
        y3[pl.ds(1 + j0, m3)] = _relu(v).astype(BF)

    def conv3(k):
        j0 = order(k) * m3
        v = sum_dots(taps(y3, j0, m3), lambda t: wc3[1, t]) + _dot(_flat(z2[pl.ds(j0 + 1, m3), 0, :, LO]), wp3[...])
        acc3[pl.ds(j0, m3)] = tiles(v, m3) + bias[5]

    def halo3(k):
        j0 = order(k) * m3
        v = sum_dots(taps(yt3, j0, m3), lambda t: wc3[0, t]) + sum_dots(taps(yb3, j0, m3), lambda t: wc3[2, t])
        v = _relu(tiles(v, m3) + acc3[pl.ds(j0, m3)])
        r = pl.ds(pl.multiple_of(j0 * IMG, IMG), m3 * IMG)
        zo[0, r] = _flat(v[:, :, LO])
        zo[1, r] = _flat(v[:, :, HI])

    last = N - 1

    def wait_next(downs, ups, k):
        if k == 0:
            recv(downs, ups, 0)
        if k < last:
            recv(downs, ups, k + 1)

    for k in range(last):
        down1(k)
    for k in range(last):
        send([m_y1d], [], k)

    for c in late_copies:
        c.wait()
    for kw in TAPS:
        toeplitz(wc1.at[kw], 4, 4, s_c1, tap_of(wc1r, kw, 1))
        toeplitz(wch1.at[kw], 2, 4, s_c1, lambda r, i: wc1r[2 * r, kw] if i == 3 * r else None)
    toeplitz(wpp1, 8, 4, s_d1, lambda r, i: wp1r[...] if r == 2 * i else None)

    s_d2, s_c2 = wd2r.shape[2:], wc2r.shape[2:]
    for kw in TAPS:
        toeplitz(wd2.at[kw], 4, 2, s_d2, tap_of(wd2r, kw, 2))
        toeplitz(wdb2.at[kw], 4, 1, s_d2, lambda r, i: wd2r[r - 1, kw] if r else None)
        toeplitz(wc2.at[kw], 2, 2, s_c2, tap_of(wc2r, kw, 1))
        toeplitz(wch2.at[kw], 2, 2, s_c2, lambda r, i: wc2r[2 * r, kw] if i == r else None)
    toeplitz(wpp2, 4, 2, s_d2, lambda r, i: wp2r[...] if r == 2 * i else None)
    toeplitz(wdh2, 4, 1, s_d2, lambda r, i: wd2r[0, r] if r in TAPS else None)

    recv([m_xtop], [], outer)
    transpose_top(outer)
    top1(0)
    send([], [m_y1u], 0)
    top1(1)
    send([], [m_y1u], 1)

    recv([m_xtop], [], inner)
    transpose_top(inner)
    top1(2)
    top1(3)
    send([], [m_y1u], 2)
    send([], [m_y1u], 3)
    conv1(0)

    def border1():
        @pl.when(has_up)
        def _():
            m_diag().wait_recv()

        for_col(lambda c: m_xcol(1 - c).wait_recv())
        unpack_diag()
        down1(last, True)
        send([m_y1d], [m_y1u], last)

    def first_z1():
        for k in range(2):
            recv([m_y1d], [m_y1u], k)
            unpack1(k)
        halo1(0)
        conv1(1)
        send([m_z1], [m_z1u], 0)

    border1()
    first_z1()

    for k in range(1, N):
        if k < last:
            recv([m_y1d], [m_y1u], k + 1)
            unpack1(k + 1)
        if k >= 2:
            down2(k - 2)
        halo1(k)
        if k < last:
            conv1(k + 1)
        send([m_z1], [m_z1u], k)
    for k in range(3):
        send([m_y2d], [], k)
    down2(3)
    down2(last)
    send([m_y2d], [], 3)
    send([m_y2d], [], last)

    def above2(k):
        if k == 0:
            recv([m_z1], [], 0)
            unpack2(0)
        if k < last:
            recv([m_z1], [], k + 1)
            unpack2(k + 1)
        if k >= 2:
            conv2(k - 2)
        top2(k)

    above2(0)
    above2(1)
    recv([], [m_z1u], 0)
    for k in range(last):
        if k + 2 < N:
            above2(k + 2)
        else:
            conv2(3)
            conv2(last)
        recv([], [m_z1u], k + 1)
        bottom2(k)
        if k == last - 1:
            bottom2(last)
        if k:
            wait_next([m_y2d], [], k - 1)
            if k == last - 1:
                down3(0)
            halo2(k - 1)
            send([m_z2], [], k - 1)
    recv([m_y2d], [], last)
    down3(1)
    halo2(3)
    halo2(last)
    send([m_z2], [], 3)
    send([m_z2], [], last)

    recv([m_z2], [], 0)
    for k in range(3):
        recv([m_z2], [], k + 1)
        top3(k)
        down3(k + 2)
        send([m_y3d], [m_y3u], k)
    recv([m_z2], [], last)
    top3(3)
    top3(last)
    send([m_y3d], [m_y3u], 3)
    send([m_y3d], [m_y3u], last)
    for k in range(N):
        conv3(k)

    half = IMG

    def write_out(h):
        lo = pl.multiple_of(half * h, half)
        for n in range(IMG):
            v = [zo[g, pl.ds(PAD * 4 * col + half * IMG * h + n, half, stride=IMG), :] for g in range(2)]
            out_ref[n, 0, pl.ds(lo, half)] = jnp.concatenate(v, axis=-1).astype(BF)

    for k in range(3):
        wait_next([m_y3d], [m_y3u], k)
    for k in range(3):
        halo3(k)
    write_out(outer)
    recv([m_y3d], [m_y3u], last)
    halo3(3)
    halo3(last)
    write_out(inner)

    for_col(lambda c: m_xcol(c).wait_send())

    @pl.when(has_down)
    def _():
        m_diag().wait_send()
        for h in range(2):
            m_xtop(h).wait_send()

        for k in range(N):
            for m in (m_y1d, m_z1, m_y2d, m_z2, m_y3d):
                m(k).wait_send()

    @pl.when(has_up)
    def _():
        for k in range(N):
            for m in (m_y1u, m_z1u, m_y3u):
                m(k).wait_send()


def solution(mesh):
    row_count = mesh.shape["row"]
    tile_spec = P("batch", "row", "col")
    c1, c2, c3 = COLS

    def vm(*shape, dtype=BF):
        return pltpu.VMEM(shape, dtype)

    def weights(cin, cout):
        return [vm(3, 3, cin, cout), vm(3, 3, cout, cout), vm(cin, cout)]

    packed = vm(c2, IMG, L)
    scratch = [
        vm(2, IMG, 8, Q, L), vm(c1 + 1, 2, IMG, LL), vm(2, IMG, Q, L), vm(c1 + 1, 2, IMG, L),
        vm(2, IMG * STEP, L, dtype=F32), vm(PAD // 2, IMG, L), vm(PAD // 2, IMG, L), vm(6, IMG, LL, dtype=F32),
        *weights(Q, H), *weights(H, L), *weights(L, LL),
        *[vm(1, c, dtype=F32) for c in (H, H, L, L, LL, LL)],
        vm(3, LL, LL), vm(L, L), vm(3, LL, LL), vm(3, L, LL), vm(LL, LL),
        vm(3, LL, LL), vm(LL, L), vm(3, LL, L), vm(3, LL, LL), vm(3, LL, LL), vm(LL, LL),
        vm(c1, IMG, L, dtype=F32), vm(c2, IMG, L, dtype=F32), vm(c3, IMG, LL, dtype=F32),
        vm(c1, IMG, LL, dtype=F32), vm(c2, IMG, LL, dtype=F32), vm(c3, IMG, LL, dtype=F32),
        vm(c1 + 2, IMG, LL), vm(c2 + 2, IMG, LL), vm(c3 + 2, IMG, LL), vm(c2 + 1, 2, IMG, LL), vm(c3 + 1, 2, IMG, LL),
        vm(2, c3 * IMG, L, dtype=F32),
        *[packed] * 6,
        vm(c1 + 2, IMG, L), vm(c2 + 2, IMG, LL), vm(c3 + 2, IMG, LL), vm(c3 + 2, IMG, LL), vm(c2 + 1, 2, IMG, L), vm(c2 + 1, 2, IMG, L), vm(c3 + 1, 2, IMG, L),
        pltpu.SemaphoreType.DMA((2,)), pltpu.SemaphoreType.DMA((15,)),
        pltpu.SemaphoreType.DMA((MESSAGES, N)), pltpu.SemaphoreType.DMA((MESSAGES, N)),
        pltpu.SemaphoreType.REGULAR,
    ]

    def local(x_tile, *params):
        x_t = jnp.transpose(x_tile, (0, 1, 3, 2))
        params = [p.reshape(1, -1) if p.ndim == 1 else p for p in params]
        operands = [pltpu.with_memory_space_constraint(p, pltpu.HBM) for p in (x_t, *params)]
        return pl.pallas_call(
            functools.partial(_body, row_count),
            out_shape=pltpu.VMEM((IMG, 1, 32, LL), BF),
            in_specs=[pl.BlockSpec(memory_space=pltpu.HBM)] * len(operands),
            out_specs=pl.BlockSpec(memory_space=pltpu.VMEM),
            scratch_shapes=scratch,
            compiler_params=pltpu.CompilerParams(collective_id=0, has_side_effects=True, vmem_limit_bytes=60 * MIB),
        )(*operands)

    return jax.shard_map(local, mesh=mesh, in_specs=(tile_spec,) + (P(),) * 15, out_specs=tile_spec, check_vma=False)
```

```python
import functools

import jax
import jax.numpy as jnp
from jax import lax
from jax.experimental import pallas as pl
from jax.experimental.pallas import tpu as pltpu
from jax.sharding import PartitionSpec as P

MESH = pl.DeviceIdType.MESH
BF = jnp.bfloat16
F32 = jnp.float32

L = 128
LL = 2 * L
H = L // 2
Q = L // 4
LO = slice(0, L)
HI = slice(L, LL)
IMG = 16
SIZES = (5, 5, 5, 6, 7, 7)
N = len(SIZES)
EDGE = 3
PAD = 12
NEED = (11, 7)
COLS = (140, 70, 35)
STEP = 132
TAPS = range(3)
MIB = 1024 * 1024

(X_TOP, DIAG, X_COL, Y1_DOWN, Y1_UP, Z1_DOWN, Y2_DOWN, Z1_UP, Z2_DOWN, Y3_DOWN, Y3_UP, MESSAGES) = range(12)
SLOT = {X_TOP: 0, DIAG: 2, X_COL: 3, **{m: 4 + N * i for i, m in enumerate((Y1_DOWN, Y1_UP, Z1_DOWN, Y2_DOWN, Z1_UP))}}
SLOT[Z2_DOWN], SLOT[Y3_UP] = SLOT[Y1_DOWN], SLOT[Y1_UP]
SLOTS = 4 + 5 * N


def _dot(a, b):
    return jnp.dot(a, b, preferred_element_type=F32)


def _flat(v):
    return v.reshape(v.shape[0] * v.shape[1], v.shape[2])


def _roll(v, shift):
    return pltpu.roll(v, shift, v.ndim - 1)


def _lane(shape):
    return lax.broadcasted_iota(jnp.int32, shape, len(shape) - 1)


def _relu(v):
    return jnp.maximum(v, 0.0)


def _body(row_count, *refs):
    (x_hbm, wd1_h, bd1_h, wc1_h, bc1_h, wp1_h, wd2_h, bd2_h, wc2_h, bc2_h, wp2_h, wd3_h, bd3_h, wc3_h, bc3_h, wp3_h,
     out_ref,
     xv, xt, xtop, xh, fs, sdiag, rdiag, bias,
     wd1r, wc1r, wp1r, wd2r, wc2r, wp2r, wd3, wc3, wp3, bd1, bc1, bd2, bc2, bd3, bc3,
     wd1, wdh1, wc1, wch1, wpp1, wd2, wdh2, wdb2, wc2, wch2, wpp2,
     part1, part2, part3, acc1, acc2, acc3, y1, y2, y3, z1, z2, zo,
     sy1d, sy1u, sz1, ry1d, ry1u, rz1,
     yh1, yh2, yt3, yb3, zh1, zb1, zh2,
     xsem, wsem, ssem, rsem, near_sem) = refs

    row = lax.axis_index("row")
    col = lax.axis_index("col")
    outer, inner = col, 1 - col
    has_up = row > 0
    has_down = row < row_count - 1
    up = {"row": row - 1}
    down = {"row": row + 1}
    side = {"col": 1 - col}
    diag_down = {"row": row + 1, "col": 1 - col}

    barrier = pltpu.get_barrier_semaphore()

    def greet(device):
        pl.semaphore_signal(barrier, inc=1, device_id=device, device_id_type=MESH)

    greet(side)

    @pl.when(has_up)
    def _():
        greet(up)

    @pl.when(has_down)
    def _():
        greet(down)

    def x_copy(h, part):
        rows = pl.ds(*((7, 1), (0, 4), (4, 3), (0, 7))[part])
        return pltpu.make_async_copy(x_hbm.at[:, rows, :, pl.ds(pl.multiple_of(h * L, L), L)], xv.at[h, :, rows],
                                     xsem.at[h, min(part, 1)])

    w_copies = [pltpu.make_async_copy(s, d, wsem.at[i]) for i, (s, d) in enumerate(
        ((wd1_h, wd1r), (bd1_h, bd1), (bc1_h, bc1), (bd2_h, bd2), (bc2_h, bc2), (bd3_h, bd3), (bc3_h, bc3),
         (wc1_h, wc1r), (wp1_h, wp1r), (wd2_h, wd2r), (wc2_h, wc2r), (wp2_h, wp2r),
         (wd3_h, wd3), (wc3_h, wc3), (wp3_h, wp3)))]
    first_copies, late_copies = w_copies[:7], w_copies[7:]
    x_copy(outer, 0).start()
    x_copy(inner, 0).start()
    for h in (inner, outer):
        for part in (1, 2):
            x_copy(h, part).start()
    for c in first_copies:
        c.start()

    def span(k, stage):
        before, scale = sum(SIZES[:k]), COLS[stage - 1] // COLS[2]
        first = before + col * (COLS[2] - SIZES[k] - 2 * before)
        return scale * first, scale * SIZES[k]

    def remote(src, dst, msg, k, dev):
        k = 0 if k is None else k
        got = wsem.at[k] if msg == Y3_DOWN else rsem.at[SLOT[msg] + k]
        return pltpu.make_async_remote_copy(src_ref=src, dst_ref=dst, send_sem=ssem.at[msg], recv_sem=got,
                                            device_id=dev, device_id_type=MESH)

    def m_xtop(h):
        if h is None:
            return remote(xtop, xtop, X_TOP, h, down)
        return remote(xv.at[h, :, 7], xtop.at[h], X_TOP, h, down)

    def m_diag():
        return remote(sdiag, rdiag, DIAG, 0, diag_down)

    own_edge = 1 + (L - PAD) * inner + PAD * col
    far_edge = 1 + L * col

    def m_xcol(c):
        skip = (PAD - NEED[0]) * (1 - c)
        return remote(xt.at[pl.ds(own_edge + skip, NEED[c])], xt.at[pl.ds(far_edge + skip, NEED[c])], X_COL, 0, side)

    def for_col(fn):
        for c in range(2):
            @pl.when(col == c)
            def _():
                fn(c)

    def chunk(k, stage, spare):
        if k is None:
            return pl.ds(1, COLS[stage - 1] - spare)
        first, size = span(k, stage)
        if k == N - 1:
            return pl.ds(1 + first + spare * col, size - spare)
        return pl.ds(1 + first, size)

    def plain(src, dst, msg, dev, stage, spare, src_lanes=None, dst_lanes=None):
        def make(k):
            s = chunk(k, stage, spare)
            return remote(src.at[s] if src_lanes is None else src.at[s, :, src_lanes],
                          dst.at[s] if dst_lanes is None else dst.at[s, :, dst_lanes], msg, k, dev)
        return make

    lanes_lo, lanes_hi = pl.ds(0, L), pl.ds(L, L)
    def packed(src, dst, msg, dev):
        def make(k):
            s = pl.ds(0, COLS[1]) if k is None else pl.ds(*span(k, 2))
            return remote(src.at[s], dst.at[s], msg, k, dev)
        return make

    m_y1d = packed(sy1d, ry1d, Y1_DOWN, down)
    m_y1u = packed(sy1u, ry1u, Y1_UP, up)
    m_z1 = packed(sz1, rz1, Z1_DOWN, down)
    m_y2d = plain(y2, yh2, Y2_DOWN, down, 2, 2, lanes_hi, lanes_lo)
    m_y3d = plain(y3, yt3, Y3_DOWN, down, 3, 2)
    m_y3u = plain(y3, yb3, Y3_UP, up, 3, 2)

    def m_z1u(k):
        s = chunk(k, 2, 1)
        return remote(z1.at[s, :, :, lanes_lo], zb1.at[s], Z1_UP, k, up)

    def m_z2(k):
        s = chunk(k, 3, 1)
        return remote(z2.at[s, :, :, lanes_hi], zh2.at[s], Z2_DOWN, k, down)

    def send(downs, ups, k):
        if downs:
            @pl.when(has_down)
            def _():
                for m in downs:
                    m(k).start()
        if ups:
            @pl.when(has_up)
            def _():
                for m in ups:
                    m(k).start()

    def recv(downs, ups, k):
        if downs:
            @pl.when(has_up)
            def _():
                for m in downs:
                    m(k).wait_recv()
        if ups:
            @pl.when(has_down)
            def _():
                for m in ups:
                    m(k).wait_recv()

    for ref in (xt, xh, z1, z2, zh1, zb1, zh2, y1, y2, y3, yh1, yh2, yt3, yb3):
        ref[0] = jnp.zeros(ref.shape[1:], BF)
    for ref in (y1, y2, y3, yh1, yh2, yt3, yb3):
        ref[ref.shape[0] - 1] = jnp.zeros(ref.shape[1:], BF)

    vertical = jnp.minimum(row, 1) + jnp.minimum(row_count - 1 - row, 1)
    pl.semaphore_wait(barrier, 1 + vertical)

    for h in (outer, inner):
        x_copy(h, 0).wait()
        send([m_xtop], [], h)
    @pl.when(has_up)
    def _():
        pl.semaphore_signal(near_sem, inc=1, device_id=up, device_id_type=MESH)

    @pl.when(has_down)
    def _():
        pl.semaphore_signal(near_sem, inc=1, device_id=down, device_id_type=MESH)

    for c in late_copies:
        c.start()

    @pl.when(jnp.logical_not(has_up))
    def _():
        for ref in (xtop, rdiag, ry1d, rz1, zh2, yt3):
            ref[...] = jnp.zeros(ref.shape, BF)
        yh2[:, :, LO] = jnp.zeros((yh2.shape[0], IMG, L), BF)

    @pl.when(jnp.logical_not(has_down))
    def _():
        for ref in (ry1u, zb1, yb3):
            ref[...] = jnp.zeros(ref.shape, BF)

    def toeplitz(dst, rows_in, rows_out, shape, piece):
        for r in range(rows_in):
            parts = []
            for i in range(rows_out):
                v = piece(r, i)
                parts.append(jnp.zeros(shape, BF) if v is None else v)
            dst[r * shape[0]:(r + 1) * shape[0], :] = jnp.concatenate(parts, axis=1)

    def tap_of(w, kw, stride):
        def piece(r, i):
            kh = r - stride * i + 1
            return w[kh, kw] if kh in TAPS else None
        return piece

    for c in first_copies:
        c.wait()
    for i, (b, reps) in enumerate(((bd1, 4), (bc1, 4), (bd2, 2), (bc2, 2), (bd3, 1), (bc3, 1))):
        v = jnp.concatenate([b[...]] * reps, axis=-1)
        bias[i] = jnp.broadcast_to(v, (IMG, LL))
    s_d1, s_c1 = wd1r.shape[2:], wc1r.shape[2:]
    for kw in TAPS:
        toeplitz(wd1.at[kw], 8, 4, s_d1, tap_of(wd1r, kw, 2))
    toeplitz(wdh1, 4, 2, s_d1, lambda r, i: wd1r[0, r] if r in TAPS and i == 0 else None)

    def transpose_half(h):
        for n in range(IMG):
            for g in range(2):
                block = xv[h, n, 4 * g:4 * g + 4].reshape(L, L)
                fs[g, n * STEP:n * STEP + L, :] = block.T.astype(F32)

    def gather_pairs(h, lo, n):
        base = 1 + PAD * col + H * h

        @pl.loop(0, n, unroll=4)
        def _(i):
            p = lo + i
            for e in range(2):
                v = [fs[g, pl.ds(2 * p + e, IMG, stride=STEP), :] for g in range(2)]
                xt[base + p, e] = jnp.concatenate(v, axis=-1).astype(BF)

    def transpose_top(h):
        for n in range(IMG):
            block = jnp.concatenate([xtop[h, n]] * 4, axis=0)
            fs[0, n * STEP:n * STEP + L, :] = block.T.astype(F32)
        base = 1 + PAD * col + H * h

        @pl.loop(0, H, unroll=8)
        def _(p):
            for e in range(2):
                xh[base + p, e] = fs[0, pl.ds(2 * p + e, IMG, stride=STEP), :].astype(BF)

    quads = (PAD // 2, 4, IMG, L)

    def pack_diag():
        v = xt[pl.ds(own_edge, PAD), :, :, HI].astype(F32).reshape(quads)
        ln = _lane((quads[0], IMG, L))
        r = v[:, 3]
        for q in TAPS:
            r = jnp.where((ln >= q * Q) & (ln < (q + 1) * Q), _roll(v[:, q], (q + 1) * Q), r)
        sdiag[...] = r.astype(BF)

    def unpack_diag():
        v = rdiag[...].astype(F32)
        ln = _lane(v.shape)
        out = []
        for q in range(4):
            r = jnp.where((ln >= q * Q) & (ln < (q + 1) * Q), v, 0.0)
            r = r + _roll(r, Q)
            out.append(r + _roll(r, H))
        u = jnp.stack(out, axis=1).astype(BF)
        xh[pl.ds(1 + L * (1 - col), PAD)] = u.reshape(PAD, 2, IMG, L)

    border = (H - PAD) * inner
    x_copy(inner, 3).wait()
    transpose_half(inner)
    gather_pairs(inner, border, PAD)
    for_col(lambda c: m_xcol(c).start())
    pack_diag()
    gather_pairs(inner, PAD * col, H - PAD)
    x_copy(outer, 3).wait()
    transpose_half(outer)
    gather_pairs(outer, 0, H)
    pl.semaphore_wait(near_sem, vertical)

    @pl.when(has_down)
    def _():
        m_diag().start()

    def taps(ref, j0, m):
        return [_flat(ref[pl.ds(j0 + t, m)]) for t in TAPS]

    def pair_taps(ref, j0, m):
        return [_flat(ref[pl.ds(j0, m), 1]), _flat(ref[pl.ds(j0 + 1, m), 0]), _flat(ref[pl.ds(j0 + 1, m), 1])]

    def sum_dots(lhs, w):
        v = _dot(lhs[0], w(0))
        for t in TAPS[1:]:
            v = v + _dot(lhs[t], w(t))
        return v

    def sum_narrow(lhs, w):
        pair = jnp.concatenate([w(0), w(1)], axis=0)
        return _dot(jnp.concatenate(lhs[:2], axis=-1), pair) + _dot(lhs[2], w(2))

    def tiles(v, m):
        return v.reshape(m, IMG, v.shape[-1])

    def pack(a, b):
        return jnp.where(_lane(a.shape) < H, a, b).astype(BF)

    def above1(j0, m):
        a, b, c = pair_taps(xh, j0, m)
        ln = _lane(a.shape)
        return tiles(_dot(jnp.where(ln < Q, a, jnp.where(ln < H, b, c)), wdh1[...]), m)

    def store_top1(k, v):
        j0, m = span(k, 1)
        p = m // 2
        lo = _relu(v + bias[0, :, LO])
        y1[pl.ds(1 + j0, m), :, LO] = lo.astype(BF)
        sy1u[pl.ds(*span(k, 2))] = pack(lo[:p], _roll(lo[p:], H))

    def down1(k, whole=False):
        j0, m = span(k, 1)
        p = m // 2
        v = tiles(sum_dots(pair_taps(xt, j0, m), lambda t: wd1[t]), m)
        if whole:
            store_top1(k, v[:, :, LO] + above1(j0, m))
        else:
            part1[pl.ds(j0, m)] = v[:, :, LO]
        hi = _relu(v[:, :, HI] + bias[0, :, HI])
        y1[pl.ds(1 + j0, m), :, HI] = hi.astype(BF)
        sy1d[pl.ds(*span(k, 2))] = pack(_roll(hi[:p], H), hi[p:])

    def top1(k):
        j0, m = span(k, 1)
        store_top1(k, above1(j0, m) + part1[pl.ds(j0, m)])

    def conv1(k):
        j0, m = span(k, 1)
        v = sum_dots(taps(y1, j0, m), lambda t: wc1[t]) + _dot(_flat(xt[pl.ds(j0 + 1, m), 0]), wpp1[...])
        acc1[pl.ds(j0, m)] = tiles(v, m) + bias[1]

    def unpack1(k):
        s, p = span(k, 2)
        j0 = span(k, 1)[0]
        t, b = ry1d[pl.ds(s, p)].astype(F32), ry1u[pl.ds(s, p)].astype(F32)
        yh1[pl.ds(1 + j0, p)] = pack(t, _roll(b, H))
        yh1[pl.ds(1 + j0 + p, p)] = pack(_roll(t, H), b)

    def halo1(k):
        j0, m = span(k, 1)
        s, p = span(k, 2)
        v = tiles(sum_narrow(taps(yh1, j0, m), lambda t: wch1[t]), m)
        v = _relu(v + acc1[pl.ds(j0, m)])
        z1[pl.ds(1 + s, p)] = v.astype(BF).reshape(p, 2, IMG, LL)
        hi = v[:, :, HI]
        sz1[pl.ds(s, p)] = pack(_roll(hi[:p], H), hi[p:])

    def down2(k):
        j0, m2 = span(k, 2)
        v = tiles(sum_dots(pair_taps(z1, j0, m2), lambda t: wd2[t]), m2)
        part2[pl.ds(j0, m2)] = v[:, :, LO]
        y2[pl.ds(1 + j0, m2), :, HI] = _relu(v[:, :, HI] + bias[2, :, HI]).astype(BF)

    def unpack2(k):
        s, p = span(k, 2)
        half = p // 2
        t = rz1[pl.ds(s, p)].astype(F32)
        u = _roll(t, H)
        zh1[pl.ds(1 + s, half)] = pack(t, u).reshape(half, 2, IMG, L)
        zh1[pl.ds(1 + s + half, half)] = pack(u, t).reshape(half, 2, IMG, L)

    def top2(k):
        j0, m2 = span(k, 2)
        a, b, c = pair_taps(zh1, j0, m2)
        t = jnp.concatenate([jnp.where(_lane(a.shape) < H, a, b), c], axis=-1)
        v = tiles(_dot(t, wdh2[...]), m2) + part2[pl.ds(j0, m2)]
        y2[pl.ds(1 + j0, m2), :, LO] = _relu(v + bias[2, :, LO]).astype(BF)

    def bottom2(k):
        j0, m2 = span(k, 2)
        own, below = pair_taps(z1, j0, m2), pair_taps(zb1, j0, m2)
        lhs = [jnp.concatenate([a[:, HI], b], axis=-1) for a, b in zip(own, below)]
        v = _relu(tiles(sum_dots(lhs, lambda t: wdb2[t]), m2) + bias[2, :, LO])
        yh2[pl.ds(1 + j0, m2), :, HI] = jnp.where(has_down, v, 0.0).astype(BF)

    def conv2(k):
        j0, m2 = span(k, 2)
        v = sum_dots(taps(y2, j0, m2), lambda t: wc2[t]) + _dot(_flat(z1[pl.ds(j0 + 1, m2), 0]), wpp2[...])
        acc2[pl.ds(j0, m2)] = tiles(v, m2) + bias[3]

    def halo2(k):
        j0, m2 = span(k, 2)
        v = tiles(sum_dots(taps(yh2, j0, m2), lambda t: wch2[t]), m2) + acc2[pl.ds(j0, m2)]
        s, p = span(k, 3)
        z2[pl.ds(1 + s, p)] = _relu(v).astype(BF).reshape(p, 2, IMG, LL)

    def down3(k):
        j0, m3 = span(k, 3)
        v = sum_dots(pair_taps(z2, j0, m3), lambda t: wd3[1:, t].reshape(LL, LL))
        part3[pl.ds(j0, m3)] = tiles(v, m3) + bias[4]

    def top3(k):
        j0, m3 = span(k, 3)
        v = tiles(sum_narrow(pair_taps(zh2, j0, m3), lambda t: wd3[0, t]), m3) + part3[pl.ds(j0, m3)]
        y3[pl.ds(1 + j0, m3)] = _relu(v).astype(BF)

    def conv3(k):
        j0, m3 = span(k, 3)
        v = sum_dots(taps(y3, j0, m3), lambda t: wc3[1, t]) + _dot(_flat(z2[pl.ds(j0 + 1, m3), 0, :, LO]), wp3[...])
        acc3[pl.ds(j0, m3)] = tiles(v, m3) + bias[5]

    def halo3(k):
        j0, m3 = span(k, 3)
        v = sum_dots(taps(yt3, j0, m3), lambda t: wc3[0, t]) + sum_dots(taps(yb3, j0, m3), lambda t: wc3[2, t])
        v = _relu(tiles(v, m3) + acc3[pl.ds(j0, m3)])
        r = pl.ds(pl.multiple_of(j0 * IMG, IMG), m3 * IMG)
        zo[0, r] = _flat(v[:, :, LO])
        zo[1, r] = _flat(v[:, :, HI])

    last = N - 1

    def wait_next(downs, ups, k):
        if k == 0:
            recv(downs, ups, 0)
        if k < last:
            recv(downs, ups, k + 1)

    for k in range(last):
        down1(k)
    for k in range(last):
        send([m_y1d], [], k)

    for c in late_copies:
        c.wait()
    for kw in TAPS:
        toeplitz(wc1.at[kw], 4, 4, s_c1, tap_of(wc1r, kw, 1))
        toeplitz(wch1.at[kw], 2, 4, s_c1, lambda r, i: wc1r[2 * r, kw] if i == 3 * r else None)
    toeplitz(wpp1, 8, 4, s_d1, lambda r, i: wp1r[...] if r == 2 * i else None)

    s_d2, s_c2 = wd2r.shape[2:], wc2r.shape[2:]
    for kw in TAPS:
        toeplitz(wd2.at[kw], 4, 2, s_d2, tap_of(wd2r, kw, 2))
        toeplitz(wdb2.at[kw], 4, 1, s_d2, lambda r, i: wd2r[r - 1, kw] if r else None)
        toeplitz(wc2.at[kw], 2, 2, s_c2, tap_of(wc2r, kw, 1))
        toeplitz(wch2.at[kw], 2, 2, s_c2, lambda r, i: wc2r[2 * r, kw] if i == r else None)
    toeplitz(wpp2, 4, 2, s_d2, lambda r, i: wp2r[...] if r == 2 * i else None)
    toeplitz(wdh2, 4, 1, s_d2, lambda r, i: wd2r[0, r] if r in TAPS else None)

    recv([m_xtop], [], outer)
    transpose_top(outer)
    for k in range(EDGE):
        top1(k)
        send([], [m_y1u], k)

    recv([m_xtop], [], inner)
    transpose_top(inner)
    for k in range(EDGE, last):
        top1(k)
    for k in range(EDGE, last):
        send([], [m_y1u], k)
    conv1(0)

    def border1():
        @pl.when(has_up)
        def _():
            m_diag().wait_recv()

        for_col(lambda c: m_xcol(1 - c).wait_recv())
        unpack_diag()
        down1(last, True)
        send([m_y1d], [m_y1u], last)

    def first_z1():
        for k in range(2):
            recv([m_y1d], [m_y1u], k)
            unpack1(k)
        halo1(0)
        conv1(1)
        send([m_z1], [m_z1u], 0)

    border1()
    first_z1()

    for k in range(1, N):
        if k < last:
            recv([m_y1d], [m_y1u], k + 1)
            unpack1(k + 1)
        if k >= 2:
            down2(k - 2)
        halo1(k)
        if k < last:
            conv1(k + 1)
        send([m_z1], [m_z1u], k)
    for k in range(N - 2):
        send([m_y2d], [], k)
    down2(last - 1)
    down2(last)
    send([m_y2d], [], last - 1)
    send([m_y2d], [], last)

    def above2(k):
        if k == 0:
            recv([m_z1], [], 0)
            unpack2(0)
        if k < last:
            recv([m_z1], [], k + 1)
            unpack2(k + 1)
        if k >= 2:
            conv2(k - 2)
        top2(k)

    above2(0)
    above2(1)
    recv([], [m_z1u], 0)
    for k in range(last):
        if k + 2 < N:
            above2(k + 2)
        else:
            conv2(last - 1)
            conv2(last)
        recv([], [m_z1u], k + 1)
        bottom2(k)
        if k == last - 1:
            bottom2(last)
        if k:
            wait_next([m_y2d], [], k - 1)
            if k >= 3:
                down3(k - 3)
            halo2(k - 1)
            send([m_z2], [], k - 1)
    recv([m_y2d], [], last)
    down3(last - 3)
    halo2(last - 1)
    halo2(last)
    send([m_z2], [], last - 1)
    send([m_z2], [], last)

    recv([m_z2], [], 0)
    for k in range(last - 1):
        recv([m_z2], [], k + 1)
        top3(k)
        if k < 3:
            down3(last - 2 + k)
        send([m_y3d], [m_y3u], k)
    recv([m_z2], [], last)
    top3(last - 1)
    top3(last)
    send([m_y3d], [m_y3u], last - 1)
    send([m_y3d], [m_y3u], last)
    for k in range(N):
        conv3(k)

    half = IMG

    def write_out(h):
        lo = pl.multiple_of(half * h, half)
        for n in range(IMG):
            v = [zo[g, pl.ds(PAD * 4 * col + half * IMG * h + n, half, stride=IMG), :] for g in range(2)]
            out_ref[n, 0, pl.ds(lo, half)] = jnp.concatenate(v, axis=-1).astype(BF)

    def sent(downs, ups):
        @pl.when(has_down)
        def _():
            for m in downs:
                m(None).wait_send()

        @pl.when(has_up)
        def _():
            for m in ups:
                m(None).wait_send()

    for_col(lambda c: m_xcol(c).wait_send())

    @pl.when(has_down)
    def _():
        m_diag().wait_send()
        m_xtop(None).wait_send()

    sent([m_y1d, m_z1, m_y2d, m_z2], [m_y1u, m_z1u])

    for k in range(last - 1):
        wait_next([m_y3d], [m_y3u], k)
    for k in range(last - 1):
        halo3(k)
    write_out(outer)
    sent([m_y3d], [m_y3u])
    recv([m_y3d], [m_y3u], last)
    halo3(last - 1)
    halo3(last)
    write_out(inner)


def solution(mesh):
    row_count = mesh.shape["row"]
    tile_spec = P("batch", "row", "col")
    c1, c2, c3 = COLS

    def vm(*shape, dtype=BF):
        return pltpu.VMEM(shape, dtype)

    def weights(cin, cout):
        return [vm(3, 3, cin, cout), vm(3, 3, cout, cout), vm(cin, cout)]

    packed = vm(c2, IMG, L)
    scratch = [
        vm(2, IMG, 8, Q, L), vm(c1 + 1, 2, IMG, LL), vm(2, IMG, Q, L), vm(c1 + 1, 2, IMG, L),
        vm(2, IMG * STEP, L, dtype=F32), vm(PAD // 2, IMG, L), vm(PAD // 2, IMG, L), vm(6, IMG, LL, dtype=F32),
        *weights(Q, H), *weights(H, L), *weights(L, LL),
        *[vm(1, c, dtype=F32) for c in (H, H, L, L, LL, LL)],
        vm(3, LL, LL), vm(L, L), vm(3, LL, LL), vm(3, L, LL), vm(LL, LL),
        vm(3, LL, LL), vm(LL, L), vm(3, LL, L), vm(3, LL, LL), vm(3, LL, LL), vm(LL, LL),
        vm(c1, IMG, L, dtype=F32), vm(c2, IMG, L, dtype=F32), vm(c3, IMG, LL, dtype=F32),
        vm(c1, IMG, LL, dtype=F32), vm(c2, IMG, LL, dtype=F32), vm(c3, IMG, LL, dtype=F32),
        vm(c1 + 2, IMG, LL), vm(c2 + 2, IMG, LL), vm(c3 + 2, IMG, LL), vm(c2 + 1, 2, IMG, LL), vm(c3 + 1, 2, IMG, LL),
        vm(2, c3 * IMG, L, dtype=F32),
        *[packed] * 6,
        vm(c1 + 2, IMG, L), vm(c2 + 2, IMG, LL), vm(c3 + 2, IMG, LL), vm(c3 + 2, IMG, LL), vm(c2 + 1, 2, IMG, L), vm(c2 + 1, 2, IMG, L), vm(c3 + 1, 2, IMG, L),
        pltpu.SemaphoreType.DMA((2, 2)), pltpu.SemaphoreType.DMA((15,)),
        pltpu.SemaphoreType.DMA((MESSAGES,)), pltpu.SemaphoreType.DMA((SLOTS,)),
        pltpu.SemaphoreType.REGULAR,
    ]

    def local(x_tile, *params):
        x_t = jnp.transpose(x_tile, (0, 1, 3, 2))
        params = [p.reshape(1, -1) if p.ndim == 1 else p for p in params]
        operands = [pltpu.with_memory_space_constraint(p, pltpu.HBM) for p in (x_t, *params)]
        return pl.pallas_call(
            functools.partial(_body, row_count),
            out_shape=pltpu.VMEM((IMG, 1, 32, LL), BF),
            in_specs=[pl.BlockSpec(memory_space=pltpu.HBM)] * len(operands),
            out_specs=pl.BlockSpec(memory_space=pltpu.VMEM),
            scratch_shapes=scratch,
            compiler_params=pltpu.CompilerParams(collective_id=0, has_side_effects=True, vmem_limit_bytes=60 * MIB),
        )(*operands)

    return jax.shard_map(local, mesh=mesh, in_specs=(tile_spec,) + (P(),) * 15, out_specs=tile_spec, check_vma=False)
```

```python
import functools

import jax
import jax.numpy as jnp
from jax import lax
from jax.experimental import pallas as pl
from jax.experimental.pallas import tpu as pltpu
from jax.sharding import PartitionSpec as P

MESH = pl.DeviceIdType.MESH
BF = jnp.bfloat16
F32 = jnp.float32

L = 128
LL = 2 * L
H = L // 2
Q = L // 4
LO = slice(0, L)
HI = slice(L, LL)
IMG = 16
SIZES = (5, 5, 5, 6, 7, 7)
N = len(SIZES)
EDGE = 3
PAD = 12
NEED = (11, 7)
COLS = (140, 70, 35)
STEP = 132
TAPS = range(3)
MIB = 1024 * 1024

(X_TOP, DIAG, X_COL, Y1_DOWN, Y1_UP, Z1_DOWN, Y2_DOWN, Z1_UP, Z2_DOWN, Y3_DOWN, Y3_UP, MESSAGES) = range(12)
SLOT = {X_TOP: (0, 1), DIAG: (2,), X_COL: (3,)}
WEIGHTS = 15
OWN = 4 + WEIGHTS
for i, m in enumerate((Y1_DOWN, Y1_UP, Z1_UP)):
    SLOT[m] = tuple(range(OWN + N * i, OWN + N * i + N))
SLOT[Z2_DOWN], SLOT[Y3_UP] = SLOT[Y1_DOWN], SLOT[Y1_UP]
SLOT[Z1_DOWN], SLOT[Y2_DOWN] = tuple(range(4, 4 + N)), tuple(range(4 + N, 4 + 2 * N))
SLOT[Y3_DOWN] = tuple(range(4 + 2 * N, OWN)) + SLOT[X_TOP] + SLOT[DIAG]
OUT = {X_TOP: 0, DIAG: 1, X_COL: 2, **{m: 3 for m in (Y1_DOWN, Z1_DOWN, Y2_DOWN, Z2_DOWN, Y3_DOWN)},
       **{m: 4 for m in (Y1_UP, Z1_UP, Y3_UP)}}
ROWS_DOWN = 8 * (2 * COLS[1] + COLS[1] - 2 + 2 * (COLS[2] - 1) + 2 * (COLS[2] - 2))
ROWS_UP = 8 * (COLS[1] + 2 * (COLS[1] - 1) + 2 * (COLS[2] - 2))
SLOTS = OWN + 3 * N


def _dot(a, b):
    return jnp.dot(a, b, preferred_element_type=F32)


def _flat(v):
    return v.reshape(v.shape[0] * v.shape[1], v.shape[2])


def _roll(v, shift):
    return pltpu.roll(v, shift, v.ndim - 1)


def _lane(shape):
    return lax.broadcasted_iota(jnp.int32, shape, len(shape) - 1)


def _relu(v):
    return jnp.maximum(v, 0.0)


def _body(row_count, *refs):
    (x_hbm, wd1_h, bd1_h, wc1_h, bc1_h, wp1_h, wd2_h, bd2_h, wc2_h, bc2_h, wp2_h, wd3_h, bd3_h, wc3_h, bc3_h, wp3_h,
     out_ref,
     xv, xt, xtop, xh, fs, sdiag, rdiag, bias,
     wd1r, wc1r, wp1r, wd2r, wc2r, wp2r, wd3, wc3, wp3, bd1, bc1, bd2, bc2, bd3, bc3,
     wd1, wdh1, wc1, wch1, wpp1, wd2, wdh2, wdb2, wc2, wch2, wpp2,
     part1, part2, part3, acc1, acc2, acc3, y1, y2, y3, z1, z2, zo,
     sy1d, sy1u, sz1, ry1d, ry1u, rz1,
     yh1, yh2, yt3, yb3, zh1, zb1, zh2,
     xsem, ssem, rsem, near_sem) = refs

    row = lax.axis_index("row")
    col = lax.axis_index("col")
    outer, inner = col, 1 - col
    has_up = row > 0
    has_down = row < row_count - 1
    up = {"row": row - 1}
    down = {"row": row + 1}
    side = {"col": 1 - col}
    diag_down = {"row": row + 1, "col": 1 - col}

    barrier = pltpu.get_barrier_semaphore()

    def greet(device):
        pl.semaphore_signal(barrier, inc=1, device_id=device, device_id_type=MESH)

    greet(side)

    @pl.when(has_up)
    def _():
        greet(up)

    @pl.when(has_down)
    def _():
        greet(down)

    def x_copy(h, part):
        rows = pl.ds(*((7, 1), (0, 4), (4, 3), (0, 7))[part])
        return pltpu.make_async_copy(x_hbm.at[:, rows, :, pl.ds(pl.multiple_of(h * L, L), L)], xv.at[h, :, rows],
                                     xsem.at[h, min(part, 1)])

    w_copies = [pltpu.make_async_copy(s, d, rsem.at[4 + i]) for i, (s, d) in enumerate(
        ((wd1_h, wd1r), (bd1_h, bd1), (bc1_h, bc1), (bd2_h, bd2), (bc2_h, bc2), (bd3_h, bd3), (bc3_h, bc3),
         (wc1_h, wc1r), (wp1_h, wp1r), (wd2_h, wd2r), (wc2_h, wc2r), (wp2_h, wp2r),
         (wd3_h, wd3), (wc3_h, wc3), (wp3_h, wp3)))]
    first_copies, late_copies = w_copies[:7], w_copies[7:]
    x_copy(outer, 0).start()
    x_copy(inner, 0).start()
    for h in (inner, outer):
        for part in (1, 2):
            x_copy(h, part).start()
    for c in first_copies:
        c.start()

    def span(k, stage):
        before, scale = sum(SIZES[:k]), COLS[stage - 1] // COLS[2]
        first = before + col * (COLS[2] - SIZES[k] - 2 * before)
        return scale * first, scale * SIZES[k]

    def remote(src, dst, msg, k, dev):
        slot = SLOT[msg][k] if isinstance(k, int) else k
        return pltpu.make_async_remote_copy(src_ref=src, dst_ref=dst, send_sem=ssem.at[OUT[msg]], recv_sem=rsem.at[slot],
                                            device_id=dev, device_id_type=MESH)

    def m_xtop(h):
        if h is None:
            return remote(xtop, xtop, X_TOP, 0, down)
        return remote(xv.at[h, :, 7], xtop.at[h], X_TOP, h, down)

    def m_diag():
        return remote(sdiag, rdiag, DIAG, 0, diag_down)

    own_edge = 1 + (L - PAD) * inner + PAD * col
    far_edge = 1 + L * col

    def m_xcol(c):
        skip = (PAD - NEED[0]) * (1 - c)
        return remote(xt.at[pl.ds(own_edge + skip, NEED[c])], xt.at[pl.ds(far_edge + skip, NEED[c])], X_COL, 0, side)

    def for_col(fn):
        for c in range(2):
            @pl.when(col == c)
            def _():
                fn(c)

    def chunk(k, stage, spare):
        first, size = span(k, stage)
        if k == N - 1:
            return pl.ds(1 + first + spare * col, size - spare)
        return pl.ds(1 + first, size)

    def plain(src, dst, msg, dev, stage, spare, src_lanes=None, dst_lanes=None):
        def make(k):
            s = chunk(k, stage, spare)
            return remote(src.at[s] if src_lanes is None else src.at[s, :, src_lanes],
                          dst.at[s] if dst_lanes is None else dst.at[s, :, dst_lanes], msg, k, dev)
        return make

    lanes_lo, lanes_hi = pl.ds(0, L), pl.ds(L, L)
    def packed(src, dst, msg, dev):
        def make(k):
            s = pl.ds(*span(k, 2))
            return remote(src.at[s], dst.at[s], msg, k, dev)
        return make

    m_y1d = packed(sy1d, ry1d, Y1_DOWN, down)
    m_y1u = packed(sy1u, ry1u, Y1_UP, up)
    m_z1 = packed(sz1, rz1, Z1_DOWN, down)
    m_y2d = plain(y2, yh2, Y2_DOWN, down, 2, 2, lanes_hi, lanes_lo)
    m_y3d = plain(y3, yt3, Y3_DOWN, down, 3, 2)
    m_y3u = plain(y3, yb3, Y3_UP, up, 3, 2)

    def m_z1u(k):
        s = chunk(k, 2, 1)
        return remote(z1.at[s, :, :, lanes_lo], zb1.at[s], Z1_UP, k, up)

    def m_z2(k):
        s = chunk(k, 3, 1)
        return remote(z2.at[s, :, :, lanes_hi], zh2.at[s], Z2_DOWN, k, down)

    def send(downs, ups, k):
        if downs:
            @pl.when(has_down)
            def _():
                for m in downs:
                    m(k).start()
        if ups:
            @pl.when(has_up)
            def _():
                for m in ups:
                    m(k).start()

    def recv(downs, ups, k):
        if downs:
            @pl.when(has_up)
            def _():
                for m in downs:
                    m(k).wait_recv()
        if ups:
            @pl.when(has_down)
            def _():
                for m in ups:
                    m(k).wait_recv()

    for ref in (xt, xh, z1, z2, zh1, zb1, zh2, y1, y2, y3, yh1, yh2, yt3, yb3):
        ref[0] = jnp.zeros(ref.shape[1:], BF)
    for ref in (y1, y2, y3, yh1, yh2, yt3, yb3):
        ref[ref.shape[0] - 1] = jnp.zeros(ref.shape[1:], BF)

    vertical = jnp.minimum(row, 1) + jnp.minimum(row_count - 1 - row, 1)
    pl.semaphore_wait(barrier, 1 + vertical)

    for h in (outer, inner):
        x_copy(h, 0).wait()
        send([m_xtop], [], h)
    @pl.when(has_up)
    def _():
        pl.semaphore_signal(near_sem, inc=1, device_id=up, device_id_type=MESH)

    @pl.when(has_down)
    def _():
        pl.semaphore_signal(near_sem, inc=1, device_id=down, device_id_type=MESH)

    for c in late_copies:
        c.start()

    @pl.when(jnp.logical_not(has_up))
    def _():
        for ref in (xtop, rdiag, ry1d, rz1, zh2, yt3):
            ref[...] = jnp.zeros(ref.shape, BF)
        yh2[:, :, LO] = jnp.zeros((yh2.shape[0], IMG, L), BF)

    @pl.when(jnp.logical_not(has_down))
    def _():
        for ref in (ry1u, zb1, yb3):
            ref[...] = jnp.zeros(ref.shape, BF)

    def toeplitz(dst, rows_in, rows_out, shape, piece):
        for r in range(rows_in):
            parts = []
            for i in range(rows_out):
                v = piece(r, i)
                parts.append(jnp.zeros(shape, BF) if v is None else v)
            dst[r * shape[0]:(r + 1) * shape[0], :] = jnp.concatenate(parts, axis=1)

    def tap_of(w, kw, stride):
        def piece(r, i):
            kh = r - stride * i + 1
            return w[kh, kw] if kh in TAPS else None
        return piece

    for c in first_copies:
        c.wait()
    for i, (b, reps) in enumerate(((bd1, 4), (bc1, 4), (bd2, 2), (bc2, 2), (bd3, 1), (bc3, 1))):
        v = jnp.concatenate([b[...]] * reps, axis=-1)
        bias[i] = jnp.broadcast_to(v, (IMG, LL))
    s_d1, s_c1 = wd1r.shape[2:], wc1r.shape[2:]
    for kw in TAPS:
        toeplitz(wd1.at[kw], 8, 4, s_d1, tap_of(wd1r, kw, 2))
    toeplitz(wdh1, 4, 2, s_d1, lambda r, i: wd1r[0, r] if r in TAPS and i == 0 else None)

    def transpose_half(h):
        for n in range(IMG):
            for g in range(2):
                block = xv[h, n, 4 * g:4 * g + 4].reshape(L, L)
                fs[g, n * STEP:n * STEP + L, :] = block.T.astype(F32)

    def gather_pairs(h, lo, n):
        base = 1 + PAD * col + H * h

        @pl.loop(0, n, unroll=4)
        def _(i):
            p = lo + i
            for e in range(2):
                v = [fs[g, pl.ds(2 * p + e, IMG, stride=STEP), :] for g in range(2)]
                xt[base + p, e] = jnp.concatenate(v, axis=-1).astype(BF)

    def transpose_top(h):
        for n in range(IMG):
            block = jnp.concatenate([xtop[h, n]] * 4, axis=0)
            fs[0, n * STEP:n * STEP + L, :] = block.T.astype(F32)
        base = 1 + PAD * col + H * h

        @pl.loop(0, H, unroll=8)
        def _(p):
            for e in range(2):
                xh[base + p, e] = fs[0, pl.ds(2 * p + e, IMG, stride=STEP), :].astype(BF)

    quads = (PAD // 2, 4, IMG, L)

    def pack_diag():
        v = xt[pl.ds(own_edge, PAD), :, :, HI].astype(F32).reshape(quads)
        ln = _lane((quads[0], IMG, L))
        r = v[:, 3]
        for q in TAPS:
            r = jnp.where((ln >= q * Q) & (ln < (q + 1) * Q), _roll(v[:, q], (q + 1) * Q), r)
        sdiag[...] = r.astype(BF)

    def unpack_diag():
        v = rdiag[...].astype(F32)
        ln = _lane(v.shape)
        out = []
        for q in range(4):
            r = jnp.where((ln >= q * Q) & (ln < (q + 1) * Q), v, 0.0)
            r = r + _roll(r, Q)
            out.append(r + _roll(r, H))
        u = jnp.stack(out, axis=1).astype(BF)
        xh[pl.ds(1 + L * (1 - col), PAD)] = u.reshape(PAD, 2, IMG, L)

    border = (H - PAD) * inner
    x_copy(inner, 3).wait()
    transpose_half(inner)
    gather_pairs(inner, border, PAD)
    for_col(lambda c: m_xcol(c).start())
    pack_diag()
    gather_pairs(inner, PAD * col, H - PAD)
    x_copy(outer, 3).wait()
    transpose_half(outer)
    gather_pairs(outer, 0, H)
    pl.semaphore_wait(near_sem, vertical)

    @pl.when(has_down)
    def _():
        m_diag().start()

    def taps(ref, j0, m):
        return [_flat(ref[pl.ds(j0 + t, m)]) for t in TAPS]

    def pair_taps(ref, j0, m):
        return [_flat(ref[pl.ds(j0, m), 1]), _flat(ref[pl.ds(j0 + 1, m), 0]), _flat(ref[pl.ds(j0 + 1, m), 1])]

    def sum_dots(lhs, w):
        v = _dot(lhs[0], w(0))
        for t in TAPS[1:]:
            v = v + _dot(lhs[t], w(t))
        return v

    def sum_narrow(lhs, w):
        pair = jnp.concatenate([w(0), w(1)], axis=0)
        return _dot(jnp.concatenate(lhs[:2], axis=-1), pair) + _dot(lhs[2], w(2))

    def tiles(v, m):
        return v.reshape(m, IMG, v.shape[-1])

    def pack(a, b):
        return jnp.where(_lane(a.shape) < H, a, b).astype(BF)

    def above1(j0, m):
        a, b, c = pair_taps(xh, j0, m)
        ln = _lane(a.shape)
        return tiles(_dot(jnp.where(ln < Q, a, jnp.where(ln < H, b, c)), wdh1[...]), m)

    def store_top1(k, v):
        j0, m = span(k, 1)
        p = m // 2
        lo = _relu(v + bias[0, :, LO])
        y1[pl.ds(1 + j0, m), :, LO] = lo.astype(BF)
        sy1u[pl.ds(*span(k, 2))] = pack(lo[:p], _roll(lo[p:], H))

    def down1(k, whole=False):
        j0, m = span(k, 1)
        p = m // 2
        v = tiles(sum_dots(pair_taps(xt, j0, m), lambda t: wd1[t]), m)
        if whole:
            store_top1(k, v[:, :, LO] + above1(j0, m))
        else:
            part1[pl.ds(j0, m)] = v[:, :, LO]
        hi = _relu(v[:, :, HI] + bias[0, :, HI])
        y1[pl.ds(1 + j0, m), :, HI] = hi.astype(BF)
        sy1d[pl.ds(*span(k, 2))] = pack(_roll(hi[:p], H), hi[p:])

    def top1(k):
        j0, m = span(k, 1)
        store_top1(k, above1(j0, m) + part1[pl.ds(j0, m)])

    def conv1(k):
        j0, m = span(k, 1)
        v = sum_dots(taps(y1, j0, m), lambda t: wc1[t]) + _dot(_flat(xt[pl.ds(j0 + 1, m), 0]), wpp1[...])
        acc1[pl.ds(j0, m)] = tiles(v, m) + bias[1]

    def unpack1(k):
        s, p = span(k, 2)
        j0 = span(k, 1)[0]
        t, b = ry1d[pl.ds(s, p)].astype(F32), ry1u[pl.ds(s, p)].astype(F32)
        yh1[pl.ds(1 + j0, p)] = pack(t, _roll(b, H))
        yh1[pl.ds(1 + j0 + p, p)] = pack(_roll(t, H), b)

    def halo1(k):
        j0, m = span(k, 1)
        s, p = span(k, 2)
        v = tiles(sum_narrow(taps(yh1, j0, m), lambda t: wch1[t]), m)
        v = _relu(v + acc1[pl.ds(j0, m)])
        z1[pl.ds(1 + s, p)] = v.astype(BF).reshape(p, 2, IMG, LL)
        hi = v[:, :, HI]
        sz1[pl.ds(s, p)] = pack(_roll(hi[:p], H), hi[p:])

    def down2(k):
        j0, m2 = span(k, 2)
        v = tiles(sum_dots(pair_taps(z1, j0, m2), lambda t: wd2[t]), m2)
        part2[pl.ds(j0, m2)] = v[:, :, LO]
        y2[pl.ds(1 + j0, m2), :, HI] = _relu(v[:, :, HI] + bias[2, :, HI]).astype(BF)

    def unpack2(k):
        s, p = span(k, 2)
        half = p // 2
        t = rz1[pl.ds(s, p)].astype(F32)
        u = _roll(t, H)
        zh1[pl.ds(1 + s, half)] = pack(t, u).reshape(half, 2, IMG, L)
        zh1[pl.ds(1 + s + half, half)] = pack(u, t).reshape(half, 2, IMG, L)

    def top2(k):
        j0, m2 = span(k, 2)
        a, b, c = pair_taps(zh1, j0, m2)
        t = jnp.concatenate([jnp.where(_lane(a.shape) < H, a, b), c], axis=-1)
        v = tiles(_dot(t, wdh2[...]), m2) + part2[pl.ds(j0, m2)]
        y2[pl.ds(1 + j0, m2), :, LO] = _relu(v + bias[2, :, LO]).astype(BF)

    def bottom2(k):
        j0, m2 = span(k, 2)
        own, below = pair_taps(z1, j0, m2), pair_taps(zb1, j0, m2)
        lhs = [jnp.concatenate([a[:, HI], b], axis=-1) for a, b in zip(own, below)]
        v = _relu(tiles(sum_dots(lhs, lambda t: wdb2[t]), m2) + bias[2, :, LO])
        yh2[pl.ds(1 + j0, m2), :, HI] = jnp.where(has_down, v, 0.0).astype(BF)

    def conv2(k):
        j0, m2 = span(k, 2)
        v = sum_dots(taps(y2, j0, m2), lambda t: wc2[t]) + _dot(_flat(z1[pl.ds(j0 + 1, m2), 0]), wpp2[...])
        acc2[pl.ds(j0, m2)] = tiles(v, m2) + bias[3]

    def halo2(k):
        j0, m2 = span(k, 2)
        v = tiles(sum_dots(taps(yh2, j0, m2), lambda t: wch2[t]), m2) + acc2[pl.ds(j0, m2)]
        s, p = span(k, 3)
        z2[pl.ds(1 + s, p)] = _relu(v).astype(BF).reshape(p, 2, IMG, LL)

    def down3(k):
        j0, m3 = span(k, 3)
        v = sum_dots(pair_taps(z2, j0, m3), lambda t: wd3[1:, t].reshape(LL, LL))
        part3[pl.ds(j0, m3)] = tiles(v, m3) + bias[4]

    def top3(k):
        j0, m3 = span(k, 3)
        v = tiles(sum_narrow(pair_taps(zh2, j0, m3), lambda t: wd3[0, t]), m3) + part3[pl.ds(j0, m3)]
        y3[pl.ds(1 + j0, m3)] = _relu(v).astype(BF)

    def conv3(k):
        j0, m3 = span(k, 3)
        v = sum_dots(taps(y3, j0, m3), lambda t: wc3[1, t]) + _dot(_flat(z2[pl.ds(j0 + 1, m3), 0, :, LO]), wp3[...])
        acc3[pl.ds(j0, m3)] = tiles(v, m3) + bias[5]

    def halo3(k):
        j0, m3 = span(k, 3)
        v = sum_dots(taps(yt3, j0, m3), lambda t: wc3[0, t]) + sum_dots(taps(yb3, j0, m3), lambda t: wc3[2, t])
        v = _relu(tiles(v, m3) + acc3[pl.ds(j0, m3)])
        r = pl.ds(pl.multiple_of(j0 * IMG, IMG), m3 * IMG)
        zo[0, r] = _flat(v[:, :, LO])
        zo[1, r] = _flat(v[:, :, HI])

    last = N - 1

    def wait_next(downs, ups, k):
        if k == 0:
            recv(downs, ups, 0)
        if k < last:
            recv(downs, ups, k + 1)

    for k in range(last):
        down1(k)
    for k in range(last):
        send([m_y1d], [], k)

    for c in late_copies:
        c.wait()
    for kw in TAPS:
        toeplitz(wc1.at[kw], 4, 4, s_c1, tap_of(wc1r, kw, 1))
        toeplitz(wch1.at[kw], 2, 4, s_c1, lambda r, i: wc1r[2 * r, kw] if i == 3 * r else None)
    toeplitz(wpp1, 8, 4, s_d1, lambda r, i: wp1r[...] if r == 2 * i else None)

    s_d2, s_c2 = wd2r.shape[2:], wc2r.shape[2:]
    for kw in TAPS:
        toeplitz(wd2.at[kw], 4, 2, s_d2, tap_of(wd2r, kw, 2))
        toeplitz(wdb2.at[kw], 4, 1, s_d2, lambda r, i: wd2r[r - 1, kw] if r else None)
        toeplitz(wc2.at[kw], 2, 2, s_c2, tap_of(wc2r, kw, 1))
        toeplitz(wch2.at[kw], 2, 2, s_c2, lambda r, i: wc2r[2 * r, kw] if i == r else None)
    toeplitz(wpp2, 4, 2, s_d2, lambda r, i: wp2r[...] if r == 2 * i else None)
    toeplitz(wdh2, 4, 1, s_d2, lambda r, i: wd2r[0, r] if r in TAPS else None)

    recv([m_xtop], [], outer)
    transpose_top(outer)
    for k in range(EDGE):
        top1(k)
        send([], [m_y1u], k)

    recv([m_xtop], [], inner)
    transpose_top(inner)
    for k in range(EDGE, last):
        top1(k)
    for k in range(EDGE, last):
        send([], [m_y1u], k)
    conv1(0)

    def border1():
        @pl.when(has_up)
        def _():
            m_diag().wait_recv()

        for_col(lambda c: m_xcol(1 - c).wait_recv())
        unpack_diag()
        down1(last, True)
        send([m_y1d], [m_y1u], last)

    def first_z1():
        for k in range(2):
            recv([m_y1d], [m_y1u], k)
            unpack1(k)
        halo1(0)
        conv1(1)
        send([m_z1], [m_z1u], 0)

    border1()
    first_z1()

    for k in range(1, N):
        if k < last:
            recv([m_y1d], [m_y1u], k + 1)
            unpack1(k + 1)
        if k >= 2:
            down2(k - 2)
        halo1(k)
        if k < last:
            conv1(k + 1)
        send([m_z1], [m_z1u], k)
    for k in range(N - 2):
        send([m_y2d], [], k)
    down2(last - 1)
    down2(last)
    send([m_y2d], [], last - 1)
    send([m_y2d], [], last)

    def above2(k):
        if k == 0:
            recv([m_z1], [], 0)
            unpack2(0)
        if k < last:
            recv([m_z1], [], k + 1)
            unpack2(k + 1)
        if k >= 2:
            conv2(k - 2)
        top2(k)

    above2(0)
    above2(1)
    recv([], [m_z1u], 0)
    for k in range(last):
        if k + 2 < N:
            above2(k + 2)
        else:
            conv2(last - 1)
            conv2(last)
        recv([], [m_z1u], k + 1)
        bottom2(k)
        if k == last - 1:
            bottom2(last)
        if k:
            wait_next([m_y2d], [], k - 1)
            if k >= 3:
                down3(k - 3)
            halo2(k - 1)
            send([m_z2], [], k - 1)
    recv([m_y2d], [], last)
    down3(last - 3)
    halo2(last - 1)
    halo2(last)
    send([m_z2], [], last - 1)
    send([m_z2], [], last)

    recv([m_z2], [], 0)
    for k in range(last - 1):
        recv([m_z2], [], k + 1)
        top3(k)
        if k < 3:
            down3(last - 2 + k)
        send([m_y3d], [m_y3u], k)
    recv([m_z2], [], last)
    top3(last - 1)
    top3(last)
    send([m_y3d], [m_y3u], last - 1)
    send([m_y3d], [m_y3u], last)
    for k in range(N):
        conv3(k)

    half = IMG

    def write_out(h):
        lo = pl.multiple_of(half * h, half)
        for n in range(IMG):
            v = [zo[g, pl.ds(PAD * 4 * col + half * IMG * h + n, half, stride=IMG), :] for g in range(2)]
            out_ref[n, 0, pl.ds(lo, half)] = jnp.concatenate(v, axis=-1).astype(BF)

    for_col(lambda c: m_xcol(c).wait_send())

    @pl.when(has_down)
    def _():
        m_diag().wait_send()
        m_xtop(None).wait_send()


    for k in range(last - 1):
        wait_next([m_y3d], [m_y3u], k)
    for k in range(last - 1):
        halo3(k)
    write_out(outer)

    def all_sent(msg, rows, dev):
        ref = fs.at[:, pl.ds(0, rows // 2)]
        remote(ref, ref, msg, 0, dev).wait_send()

    @pl.when(has_down)
    def _():
        all_sent(Y1_DOWN, ROWS_DOWN, down)

    @pl.when(has_up)
    def _():
        all_sent(Y1_UP, ROWS_UP, up)

    recv([m_y3d], [m_y3u], last)
    halo3(last - 1)
    halo3(last)
    write_out(inner)


def solution(mesh):
    row_count = mesh.shape["row"]
    tile_spec = P("batch", "row", "col")
    c1, c2, c3 = COLS

    def vm(*shape, dtype=BF):
        return pltpu.VMEM(shape, dtype)

    def weights(cin, cout):
        return [vm(3, 3, cin, cout), vm(3, 3, cout, cout), vm(cin, cout)]

    packed = vm(c2, IMG, L)
    scratch = [
        vm(2, IMG, 8, Q, L), vm(c1 + 1, 2, IMG, LL), vm(2, IMG, Q, L), vm(c1 + 1, 2, IMG, L),
        vm(2, IMG * STEP, L, dtype=F32), vm(PAD // 2, IMG, L), vm(PAD // 2, IMG, L), vm(6, IMG, LL, dtype=F32),
        *weights(Q, H), *weights(H, L), *weights(L, LL),
        *[vm(1, c, dtype=F32) for c in (H, H, L, L, LL, LL)],
        vm(3, LL, LL), vm(L, L), vm(3, LL, LL), vm(3, L, LL), vm(LL, LL),
        vm(3, LL, LL), vm(LL, L), vm(3, LL, L), vm(3, LL, LL), vm(3, LL, LL), vm(LL, LL),
        vm(c1, IMG, L, dtype=F32), vm(c2, IMG, L, dtype=F32), vm(c3, IMG, LL, dtype=F32),
        vm(c1, IMG, LL, dtype=F32), vm(c2, IMG, LL, dtype=F32), vm(c3, IMG, LL, dtype=F32),
        vm(c1 + 2, IMG, LL), vm(c2 + 2, IMG, LL), vm(c3 + 2, IMG, LL), vm(c2 + 1, 2, IMG, LL), vm(c3 + 1, 2, IMG, LL),
        vm(2, c3 * IMG, L, dtype=F32),
        *[packed] * 6,
        vm(c1 + 2, IMG, L), vm(c2 + 2, IMG, LL), vm(c3 + 2, IMG, LL), vm(c3 + 2, IMG, LL), vm(c2 + 1, 2, IMG, L), vm(c2 + 1, 2, IMG, L), vm(c3 + 1, 2, IMG, L),
        pltpu.SemaphoreType.DMA((2, 2)), pltpu.SemaphoreType.DMA((5,)), pltpu.SemaphoreType.DMA((SLOTS,)),
        pltpu.SemaphoreType.REGULAR,
    ]

    def local(x_tile, *params):
        x_t = jnp.transpose(x_tile, (0, 1, 3, 2))
        params = [p.reshape(1, -1) if p.ndim == 1 else p for p in params]
        operands = [pltpu.with_memory_space_constraint(p, pltpu.HBM) for p in (x_t, *params)]
        return pl.pallas_call(
            functools.partial(_body, row_count),
            out_shape=pltpu.VMEM((IMG, 1, 32, LL), BF),
            in_specs=[pl.BlockSpec(memory_space=pltpu.HBM)] * len(operands),
            out_specs=pl.BlockSpec(memory_space=pltpu.VMEM),
            scratch_shapes=scratch,
            compiler_params=pltpu.CompilerParams(collective_id=0, has_side_effects=True, vmem_limit_bytes=60 * MIB),
        )(*operands)

    return jax.shard_map(local, mesh=mesh, in_specs=(tile_spec,) + (P(),) * 15, out_specs=tile_spec, check_vma=False)
```

```python
import functools

import jax
import jax.numpy as jnp
from jax import lax
from jax.experimental import pallas as pl
from jax.experimental.pallas import tpu as pltpu
from jax.sharding import PartitionSpec as P

MESH = pl.DeviceIdType.MESH
BF = jnp.bfloat16
F32 = jnp.float32

L = 128
LL = 2 * L
H = L // 2
Q = L // 4
LO = slice(0, L)
HI = slice(L, LL)
IMG = 16
SIZES = (5, 5, 5, 6, 7, 7)
N = len(SIZES)
EDGE = 3
PAD = 12
NEED = (11, 7)
COLS = (140, 70, 35)
STEP = 132
TAPS = range(3)
MIB = 1024 * 1024

(X_TOP, DIAG, X_COL, Y1_DOWN, Y1_UP, Z1_DOWN, Y2_DOWN, Z1_UP, Z2_DOWN, Y3_DOWN, Y3_UP, MESSAGES) = range(12)
SLOT = {X_TOP: (0, 1), DIAG: (2,), X_COL: (3,)}
WEIGHTS = 15
OWN = 4 + WEIGHTS
for i, m in enumerate((Y1_DOWN, Y1_UP, Z1_UP)):
    SLOT[m] = tuple(range(OWN + N * i, OWN + N * i + N))
SLOT[Z2_DOWN], SLOT[Y3_UP] = SLOT[Y1_DOWN], SLOT[Y1_UP]
SLOT[Z1_DOWN], SLOT[Y2_DOWN] = tuple(range(4, 4 + N)), tuple(range(4 + N, 4 + 2 * N))
SLOT[Y3_DOWN] = tuple(range(4 + 2 * N, OWN)) + SLOT[X_TOP] + SLOT[DIAG]
OUT = {X_TOP: 0, DIAG: 1, X_COL: 2, **{m: 3 for m in (Y1_DOWN, Z1_DOWN, Y2_DOWN, Z2_DOWN, Y3_DOWN)},
       **{m: 4 for m in (Y1_UP, Z1_UP, Y3_UP)}}
ROWS_DOWN = 8 * (2 * COLS[1] + COLS[1] - 2 + 2 * (COLS[2] - 1) + 2 * (COLS[2] - 2))
ROWS_UP = 8 * (COLS[1] + 2 * (COLS[1] - 1) + 2 * (COLS[2] - 2))
SLOTS = OWN + 3 * N


def _dot(a, b):
    return jnp.dot(a, b, preferred_element_type=F32)


def _flat(v):
    return v.reshape(v.shape[0] * v.shape[1], v.shape[2])


def _roll(v, shift):
    return pltpu.roll(v, shift, v.ndim - 1)


def _lane(shape):
    return lax.broadcasted_iota(jnp.int32, shape, len(shape) - 1)


def _relu(v):
    return jnp.maximum(v, 0.0)


def _body(row_count, *refs):
    (x_hbm, wd1_h, bd1_h, wc1_h, bc1_h, wp1_h, wd2_h, bd2_h, wc2_h, bc2_h, wp2_h, wd3_h, bd3_h, wc3_h, bc3_h, wp3_h,
     out_ref,
     xv, xt, xtop, xh, fs, sdiag, rdiag, bias,
     wd1r, wc1r, wp1r, wd2r, wc2r, wp2r, wd3, wc3, wp3, bd1, bc1, bd2, bc2, bd3, bc3,
     wd1, wdh1, wc1, wch1, wpp1, wd2, wdh2, wdb2, wc2, wch2, wpp2,
     part1, part2, part3, acc1, acc2, acc3, y1, y2, y3, z1, z2, zo,
     sy1d, sy1u, sz1, ry1d, ry1u, rz1,
     yh1, yh2, yt3, yb3, zh1, zb1, zh2,
     xsem, ssem, rsem, near_sem) = refs

    row = lax.axis_index("row")
    col = lax.axis_index("col")
    outer, inner = col, 1 - col
    has_up = row > 0
    has_down = row < row_count - 1
    up = {"row": row - 1}
    down = {"row": row + 1}
    side = {"col": 1 - col}
    diag_down = {"row": row + 1, "col": 1 - col}

    barrier = pltpu.get_barrier_semaphore()

    def greet(device):
        pl.semaphore_signal(barrier, inc=1, device_id=device, device_id_type=MESH)

    greet(side)

    @pl.when(has_up)
    def _():
        greet(up)

    @pl.when(has_down)
    def _():
        greet(down)

    def x_copy(h, part):
        rows = pl.ds(*((7, 1), (0, 4), (4, 3), (0, 7))[part])
        return pltpu.make_async_copy(x_hbm.at[:, rows, :, pl.ds(pl.multiple_of(h * L, L), L)], xv.at[h, :, rows],
                                     xsem.at[h, min(part, 1)])

    w_copies = [pltpu.make_async_copy(s, d, rsem.at[4 + i]) for i, (s, d) in enumerate(
        ((wd1_h, wd1r), (bd1_h, bd1), (bc1_h, bc1), (bd2_h, bd2), (bc2_h, bc2), (bd3_h, bd3), (bc3_h, bc3),
         (wc1_h, wc1r), (wp1_h, wp1r), (wd2_h, wd2r), (wc2_h, wc2r), (wp2_h, wp2r),
         (wd3_h, wd3), (wc3_h, wc3), (wp3_h, wp3)))]
    first_copies, late_copies = w_copies[:7], w_copies[7:]
    x_copy(outer, 0).start()
    x_copy(inner, 0).start()
    for h in (inner, outer):
        for part in (1, 2):
            x_copy(h, part).start()
    for c in first_copies:
        c.start()

    def span(k, stage):
        before, scale = sum(SIZES[:k]), COLS[stage - 1] // COLS[2]
        first = before + col * (COLS[2] - SIZES[k] - 2 * before)
        return scale * first, scale * SIZES[k]

    def remote(src, dst, msg, k, dev):
        slot = SLOT[msg][k] if isinstance(k, int) else k
        return pltpu.make_async_remote_copy(src_ref=src, dst_ref=dst, send_sem=ssem.at[OUT[msg]], recv_sem=rsem.at[slot],
                                            device_id=dev, device_id_type=MESH)

    def m_xtop(h):
        if h is None:
            return remote(xtop, xtop, X_TOP, 0, down)
        return remote(xv.at[h, :, 7], xtop.at[h], X_TOP, h, down)

    def m_diag():
        return remote(sdiag, rdiag, DIAG, 0, diag_down)

    own_edge = 1 + (L - PAD) * inner + PAD * col
    far_edge = 1 + L * col

    def m_xcol(c):
        skip = (PAD - NEED[0]) * (1 - c)
        return remote(xt.at[pl.ds(own_edge + skip, NEED[c])], xt.at[pl.ds(far_edge + skip, NEED[c])], X_COL, 0, side)

    def for_col(fn):
        for c in range(2):
            @pl.when(col == c)
            def _():
                fn(c)

    def chunk(k, stage, spare):
        first, size = span(k, stage)
        if k == N - 1:
            return pl.ds(1 + first + spare * col, size - spare)
        return pl.ds(1 + first, size)

    def plain(src, dst, msg, dev, stage, spare, src_lanes=None, dst_lanes=None):
        def make(k):
            s = chunk(k, stage, spare)
            return remote(src.at[s] if src_lanes is None else src.at[s, :, src_lanes],
                          dst.at[s] if dst_lanes is None else dst.at[s, :, dst_lanes], msg, k, dev)
        return make

    lanes_lo, lanes_hi = pl.ds(0, L), pl.ds(L, L)
    def packed(src, dst, msg, dev):
        def make(k):
            s = pl.ds(*span(k, 2))
            return remote(src.at[s], dst.at[s], msg, k, dev)
        return make

    m_y1d = packed(sy1d, ry1d, Y1_DOWN, down)
    m_y1u = packed(sy1u, ry1u, Y1_UP, up)
    m_z1 = packed(sz1, rz1, Z1_DOWN, down)
    m_y2d = plain(y2, yh2, Y2_DOWN, down, 2, 2, lanes_hi, lanes_lo)
    m_y3d = plain(y3, yt3, Y3_DOWN, down, 3, 2)
    m_y3u = plain(y3, yb3, Y3_UP, up, 3, 2)

    def m_z1u(k):
        s = chunk(k, 2, 1)
        return remote(z1.at[s, :, :, lanes_lo], zb1.at[s], Z1_UP, k, up)

    def m_z2(k):
        s = chunk(k, 3, 1)
        return remote(z2.at[s, :, :, lanes_hi], zh2.at[s], Z2_DOWN, k, down)

    def send(downs, ups, k):
        if downs:
            @pl.when(has_down)
            def _():
                for m in downs:
                    m(k).start()
        if ups:
            @pl.when(has_up)
            def _():
                for m in ups:
                    m(k).start()

    def recv(downs, ups, k):
        if downs:
            @pl.when(has_up)
            def _():
                for m in downs:
                    m(k).wait_recv()
        if ups:
            @pl.when(has_down)
            def _():
                for m in ups:
                    m(k).wait_recv()

    for ref in (xt, xh, z1, z2, zh1, zb1, zh2, y1, y2, y3, yh1, yh2, yt3, yb3):
        ref[0] = jnp.zeros(ref.shape[1:], BF)
    for ref in (y1, y2, y3, yh1, yh2, yt3, yb3):
        ref[ref.shape[0] - 1] = jnp.zeros(ref.shape[1:], BF)

    vertical = jnp.minimum(row, 1) + jnp.minimum(row_count - 1 - row, 1)
    pl.semaphore_wait(barrier, 1 + vertical)

    for h in (outer, inner):
        x_copy(h, 0).wait()
        send([m_xtop], [], h)
    @pl.when(has_up)
    def _():
        pl.semaphore_signal(near_sem, inc=1, device_id=up, device_id_type=MESH)

    @pl.when(has_down)
    def _():
        pl.semaphore_signal(near_sem, inc=1, device_id=down, device_id_type=MESH)

    for c in late_copies:
        c.start()

    @pl.when(jnp.logical_not(has_up))
    def _():
        for ref in (xtop, rdiag, ry1d, rz1, zh2, yt3):
            ref[...] = jnp.zeros(ref.shape, BF)
        yh2[:, :, LO] = jnp.zeros((yh2.shape[0], IMG, L), BF)

    @pl.when(jnp.logical_not(has_down))
    def _():
        for ref in (ry1u, zb1, yb3):
            ref[...] = jnp.zeros(ref.shape, BF)

    def toeplitz(dst, rows_in, rows_out, shape, piece):
        for r in range(rows_in):
            parts = []
            for i in range(rows_out):
                v = piece(r, i)
                parts.append(jnp.zeros(shape, BF) if v is None else v)
            dst[r * shape[0]:(r + 1) * shape[0], :] = jnp.concatenate(parts, axis=1)

    def tap_of(w, kw, stride):
        def piece(r, i):
            kh = r - stride * i + 1
            return w[kh, kw] if kh in TAPS else None
        return piece

    for c in first_copies:
        c.wait()
    for i, (b, reps) in enumerate(((bd1, 4), (bc1, 4), (bd2, 2), (bc2, 2), (bd3, 1), (bc3, 1))):
        v = jnp.concatenate([b[...]] * reps, axis=-1)
        bias[i] = jnp.broadcast_to(v, (IMG, LL))
    s_d1, s_c1 = wd1r.shape[2:], wc1r.shape[2:]
    for kw in TAPS:
        toeplitz(wd1.at[kw], 8, 4, s_d1, tap_of(wd1r, kw, 2))
    toeplitz(wdh1, 4, 2, s_d1, lambda r, i: wd1r[0, r] if r in TAPS and i == 0 else None)

    def transpose_half(h):
        for n in range(IMG):
            for g in range(2):
                block = xv[h, n, 4 * g:4 * g + 4].reshape(L, L)
                fs[g, n * STEP:n * STEP + L, :] = block.T.astype(F32)

    def gather_pairs(h, lo, n):
        base = 1 + PAD * col + H * h

        @pl.loop(0, n, unroll=4)
        def _(i):
            p = lo + i
            for e in range(2):
                v = [fs[g, pl.ds(2 * p + e, IMG, stride=STEP), :] for g in range(2)]
                xt[base + p, e] = jnp.concatenate(v, axis=-1).astype(BF)

    def transpose_top(h):
        for n in range(IMG):
            block = jnp.concatenate([xtop[h, n]] * 4, axis=0)
            fs[0, n * STEP:n * STEP + L, :] = block.T.astype(F32)
        base = 1 + PAD * col + H * h

        @pl.loop(0, H, unroll=8)
        def _(p):
            for e in range(2):
                xh[base + p, e] = fs[0, pl.ds(2 * p + e, IMG, stride=STEP), :].astype(BF)

    quads = (PAD // 2, 4, IMG, L)

    def pack_diag():
        v = xt[pl.ds(own_edge, PAD), :, :, HI].astype(F32).reshape(quads)
        ln = _lane((quads[0], IMG, L))
        r = v[:, 3]
        for q in TAPS:
            r = jnp.where((ln >= q * Q) & (ln < (q + 1) * Q), _roll(v[:, q], (q + 1) * Q), r)
        sdiag[...] = r.astype(BF)

    def unpack_diag():
        v = rdiag[...].astype(F32)
        ln = _lane(v.shape)
        out = []
        for q in range(4):
            r = jnp.where((ln >= q * Q) & (ln < (q + 1) * Q), v, 0.0)
            r = r + _roll(r, Q)
            out.append(r + _roll(r, H))
        u = jnp.stack(out, axis=1).astype(BF)
        xh[pl.ds(1 + L * (1 - col), PAD)] = u.reshape(PAD, 2, IMG, L)

    border = (H - PAD) * inner
    x_copy(inner, 3).wait()
    transpose_half(inner)
    gather_pairs(inner, border, PAD)
    for_col(lambda c: m_xcol(c).start())
    pack_diag()
    gather_pairs(inner, PAD * col, H - PAD)
    x_copy(outer, 3).wait()
    transpose_half(outer)
    gather_pairs(outer, 0, H)
    pl.semaphore_wait(near_sem, vertical)

    @pl.when(has_down)
    def _():
        m_diag().start()

    def taps(ref, j0, m):
        return [_flat(ref[pl.ds(j0 + t, m)]) for t in TAPS]

    def pair_taps(ref, j0, m):
        return [_flat(ref[pl.ds(j0, m), 1]), _flat(ref[pl.ds(j0 + 1, m), 0]), _flat(ref[pl.ds(j0 + 1, m), 1])]

    def sum_dots(lhs, w):
        v = _dot(lhs[0], w(0))
        for t in TAPS[1:]:
            v = v + _dot(lhs[t], w(t))
        return v

    def sum_narrow(lhs, w):
        pair = jnp.concatenate([w(0), w(1)], axis=0)
        return _dot(jnp.concatenate(lhs[:2], axis=-1), pair) + _dot(lhs[2], w(2))

    def tiles(v, m):
        return v.reshape(m, IMG, v.shape[-1])

    def pack(a, b):
        return jnp.where(_lane(a.shape) < H, a, b).astype(BF)

    def above1(j0, m):
        a, b, c = pair_taps(xh, j0, m)
        ln = _lane(a.shape)
        return tiles(_dot(jnp.where(ln < Q, a, jnp.where(ln < H, b, c)), wdh1[...]), m)

    def store_top1(k, v):
        j0, m = span(k, 1)
        p = m // 2
        lo = _relu(v + bias[0, :, LO])
        y1[pl.ds(1 + j0, m), :, LO] = lo.astype(BF)
        sy1u[pl.ds(*span(k, 2))] = pack(lo[:p], _roll(lo[p:], H))

    def down1(k, whole=False):
        j0, m = span(k, 1)
        p = m // 2
        v = tiles(sum_dots(pair_taps(xt, j0, m), lambda t: wd1[t]), m)
        if whole:
            store_top1(k, v[:, :, LO] + above1(j0, m))
        else:
            part1[pl.ds(j0, m)] = v[:, :, LO]
        hi = _relu(v[:, :, HI] + bias[0, :, HI])
        y1[pl.ds(1 + j0, m), :, HI] = hi.astype(BF)
        sy1d[pl.ds(*span(k, 2))] = pack(_roll(hi[:p], H), hi[p:])

    def top1(k):
        j0, m = span(k, 1)
        store_top1(k, above1(j0, m) + part1[pl.ds(j0, m)])

    def conv1(k):
        j0, m = span(k, 1)
        v = sum_dots(taps(y1, j0, m), lambda t: wc1[t]) + _dot(_flat(xt[pl.ds(j0 + 1, m), 0]), wpp1[...])
        acc1[pl.ds(j0, m)] = tiles(v, m) + bias[1]

    def unpack1(k):
        s, p = span(k, 2)
        j0 = span(k, 1)[0]
        t, b = ry1d[pl.ds(s, p)].astype(F32), ry1u[pl.ds(s, p)].astype(F32)
        yh1[pl.ds(1 + j0, p)] = pack(t, _roll(b, H))
        yh1[pl.ds(1 + j0 + p, p)] = pack(_roll(t, H), b)

    def halo1(k):
        j0, m = span(k, 1)
        s, p = span(k, 2)
        v = tiles(sum_narrow(taps(yh1, j0, m), lambda t: wch1[t]), m)
        v = _relu(v + acc1[pl.ds(j0, m)])
        z1[pl.ds(1 + s, p)] = v.astype(BF).reshape(p, 2, IMG, LL)
        hi = v[:, :, HI]
        sz1[pl.ds(s, p)] = pack(_roll(hi[:p], H), hi[p:])

    def down2(k):
        j0, m2 = span(k, 2)
        v = tiles(sum_dots(pair_taps(z1, j0, m2), lambda t: wd2[t]), m2)
        part2[pl.ds(j0, m2)] = v[:, :, LO]
        y2[pl.ds(1 + j0, m2), :, HI] = _relu(v[:, :, HI] + bias[2, :, HI]).astype(BF)

    def unpack2(k):
        s, p = span(k, 2)
        half = p // 2
        t = rz1[pl.ds(s, p)].astype(F32)
        u = _roll(t, H)
        zh1[pl.ds(1 + s, half)] = pack(t, u).reshape(half, 2, IMG, L)
        zh1[pl.ds(1 + s + half, half)] = pack(u, t).reshape(half, 2, IMG, L)

    def top2(k):
        j0, m2 = span(k, 2)
        a, b, c = pair_taps(zh1, j0, m2)
        t = jnp.concatenate([jnp.where(_lane(a.shape) < H, a, b), c], axis=-1)
        v = tiles(_dot(t, wdh2[...]), m2) + part2[pl.ds(j0, m2)]
        y2[pl.ds(1 + j0, m2), :, LO] = _relu(v + bias[2, :, LO]).astype(BF)

    def bottom2(k):
        j0, m2 = span(k, 2)
        own, below = pair_taps(z1, j0, m2), pair_taps(zb1, j0, m2)
        lhs = [jnp.concatenate([a[:, HI], b], axis=-1) for a, b in zip(own, below)]
        v = _relu(tiles(sum_dots(lhs, lambda t: wdb2[t]), m2) + bias[2, :, LO])
        yh2[pl.ds(1 + j0, m2), :, HI] = jnp.where(has_down, v, 0.0).astype(BF)

    def conv2(k):
        j0, m2 = span(k, 2)
        v = sum_dots(taps(y2, j0, m2), lambda t: wc2[t]) + _dot(_flat(z1[pl.ds(j0 + 1, m2), 0]), wpp2[...])
        acc2[pl.ds(j0, m2)] = tiles(v, m2) + bias[3]

    def halo2(k):
        j0, m2 = span(k, 2)
        v = tiles(sum_dots(taps(yh2, j0, m2), lambda t: wch2[t]), m2) + acc2[pl.ds(j0, m2)]
        s, p = span(k, 3)
        z2[pl.ds(1 + s, p)] = _relu(v).astype(BF).reshape(p, 2, IMG, LL)

    def down3(k):
        j0, m3 = span(k, 3)
        v = sum_dots(pair_taps(z2, j0, m3), lambda t: wd3[1:, t].reshape(LL, LL))
        part3[pl.ds(j0, m3)] = tiles(v, m3) + bias[4]

    def top3(k):
        j0, m3 = span(k, 3)
        v = tiles(sum_narrow(pair_taps(zh2, j0, m3), lambda t: wd3[0, t]), m3) + part3[pl.ds(j0, m3)]
        y3[pl.ds(1 + j0, m3)] = _relu(v).astype(BF)

    def conv3(k):
        j0, m3 = span(k, 3)
        v = sum_dots(taps(y3, j0, m3), lambda t: wc3[1, t]) + _dot(_flat(z2[pl.ds(j0 + 1, m3), 0, :, LO]), wp3[...])
        acc3[pl.ds(j0, m3)] = tiles(v, m3) + bias[5]

    def halo3(k):
        j0, m3 = span(k, 3)
        v = sum_dots(taps(yt3, j0, m3), lambda t: wc3[0, t]) + sum_dots(taps(yb3, j0, m3), lambda t: wc3[2, t])
        v = _relu(tiles(v, m3) + acc3[pl.ds(j0, m3)])
        r = pl.ds(pl.multiple_of(j0 * IMG, IMG), m3 * IMG)
        zo[0, r] = _flat(v[:, :, LO])
        zo[1, r] = _flat(v[:, :, HI])

    last = N - 1

    def wait_next(downs, ups, k):
        if k == 0:
            recv(downs, ups, 0)
        if k < last:
            recv(downs, ups, k + 1)

    for k in range(last):
        down1(k)
    for k in range(last):
        send([m_y1d], [], k)

    for c in late_copies:
        c.wait()
    for kw in TAPS:
        toeplitz(wc1.at[kw], 4, 4, s_c1, tap_of(wc1r, kw, 1))
        toeplitz(wch1.at[kw], 2, 4, s_c1, lambda r, i: wc1r[2 * r, kw] if i == 3 * r else None)
    toeplitz(wpp1, 8, 4, s_d1, lambda r, i: wp1r[...] if r == 2 * i else None)

    s_d2, s_c2 = wd2r.shape[2:], wc2r.shape[2:]
    for kw in TAPS:
        toeplitz(wd2.at[kw], 4, 2, s_d2, tap_of(wd2r, kw, 2))
        toeplitz(wdb2.at[kw], 4, 1, s_d2, lambda r, i: wd2r[r - 1, kw] if r else None)
        toeplitz(wc2.at[kw], 2, 2, s_c2, tap_of(wc2r, kw, 1))
        toeplitz(wch2.at[kw], 2, 2, s_c2, lambda r, i: wc2r[2 * r, kw] if i == r else None)
    toeplitz(wpp2, 4, 2, s_d2, lambda r, i: wp2r[...] if r == 2 * i else None)
    toeplitz(wdh2, 4, 1, s_d2, lambda r, i: wd2r[0, r] if r in TAPS else None)

    recv([m_xtop], [], outer)
    transpose_top(outer)
    for k in range(EDGE):
        top1(k)
        send([], [m_y1u], k)

    recv([m_xtop], [], inner)
    transpose_top(inner)
    for k in range(EDGE, last):
        top1(k)
    for k in range(EDGE, last):
        send([], [m_y1u], k)
    conv1(0)

    def border1():
        @pl.when(has_up)
        def _():
            m_diag().wait_recv()

        for_col(lambda c: m_xcol(1 - c).wait_recv())
        unpack_diag()
        down1(last, True)
        send([m_y1d], [m_y1u], last)

    def first_z1():
        for k in range(2):
            recv([m_y1d], [m_y1u], k)
            unpack1(k)
        halo1(0)
        conv1(1)
        send([m_z1], [m_z1u], 0)

    border1()
    first_z1()

    for k in range(1, N):
        if k < last:
            recv([m_y1d], [m_y1u], k + 1)
            unpack1(k + 1)
        if k >= 2:
            down2(k - 2)
        halo1(k)
        if k < last:
            conv1(k + 1)
        send([m_z1], [m_z1u], k)
    for k in range(N - 2):
        send([m_y2d], [], k)
    down2(last - 1)
    down2(last)
    send([m_y2d], [], last - 1)
    send([m_y2d], [], last)

    def above2(k):
        if k == 0:
            recv([m_z1], [], 0)
            unpack2(0)
        if k < last:
            recv([m_z1], [], k + 1)
            unpack2(k + 1)
        if k >= 2:
            conv2(k - 2)
        top2(k)

    def recv_left(m, k):
        if k == 0:
            recv([m], [], 0)
        else:
            @pl.when(jnp.logical_and(has_up, col == 0))
            def _():
                m(k).wait_recv()
        if k < last:
            @pl.when(jnp.logical_and(has_up, col == 1))
            def _():
                m(k + 1).wait_recv()

    above2(0)
    above2(1)
    recv([], [m_z1u], 0)
    for k in range(last):
        if k + 2 < N:
            above2(k + 2)
        else:
            conv2(last - 1)
            conv2(last)
        if k == last - 1:
            recv_left(m_z2, 0)
            top3(0)
            send([m_y3d], [m_y3u], 0)
        recv([], [m_z1u], k + 1)
        bottom2(k)
        if k == last - 1:
            bottom2(last)
        if k:
            wait_next([m_y2d], [], k - 1)
            if k >= 3:
                down3(k - 3)
            halo2(k - 1)
            send([m_z2], [], k - 1)
    recv([m_y2d], [], last)
    down3(last - 3)
    halo2(last - 1)
    halo2(last)
    send([m_z2], [], last - 1)
    send([m_z2], [], last)

    for k in range(1, N):
        recv_left(m_z2, k)
        top3(k)
        if k < 4:
            down3(last - 3 + k)
        send([m_y3d], [m_y3u], k)
    for k in range(N):
        conv3(k)

    half = IMG

    def write_out(h):
        lo = pl.multiple_of(half * h, half)
        for n in range(IMG):
            v = [zo[g, pl.ds(PAD * 4 * col + half * IMG * h + n, half, stride=IMG), :] for g in range(2)]
            out_ref[n, 0, pl.ds(lo, half)] = jnp.concatenate(v, axis=-1).astype(BF)

    for_col(lambda c: m_xcol(c).wait_send())

    @pl.when(has_down)
    def _():
        m_diag().wait_send()
        m_xtop(None).wait_send()


    for k in range(last - 1):
        wait_next([m_y3d], [m_y3u], k)
        halo3(k)
    write_out(outer)

    def all_sent(msg, rows, dev):
        ref = fs.at[:, pl.ds(0, rows // 2)]
        remote(ref, ref, msg, 0, dev).wait_send()

    @pl.when(has_down)
    def _():
        all_sent(Y1_DOWN, ROWS_DOWN, down)

    @pl.when(has_up)
    def _():
        all_sent(Y1_UP, ROWS_UP, up)

    recv([m_y3d], [m_y3u], last)
    halo3(last - 1)
    halo3(last)
    write_out(inner)


def solution(mesh):
    row_count = mesh.shape["row"]
    tile_spec = P("batch", "row", "col")
    c1, c2, c3 = COLS

    def vm(*shape, dtype=BF):
        return pltpu.VMEM(shape, dtype)

    def weights(cin, cout):
        return [vm(3, 3, cin, cout), vm(3, 3, cout, cout), vm(cin, cout)]

    packed = vm(c2, IMG, L)
    scratch = [
        vm(2, IMG, 8, Q, L), vm(c1 + 1, 2, IMG, LL), vm(2, IMG, Q, L), vm(c1 + 1, 2, IMG, L),
        vm(2, IMG * STEP, L, dtype=F32), vm(PAD // 2, IMG, L), vm(PAD // 2, IMG, L), vm(6, IMG, LL, dtype=F32),
        *weights(Q, H), *weights(H, L), *weights(L, LL),
        *[vm(1, c, dtype=F32) for c in (H, H, L, L, LL, LL)],
        vm(3, LL, LL), vm(L, L), vm(3, LL, LL), vm(3, L, LL), vm(LL, LL),
        vm(3, LL, LL), vm(LL, L), vm(3, LL, L), vm(3, LL, LL), vm(3, LL, LL), vm(LL, LL),
        vm(c1, IMG, L, dtype=F32), vm(c2, IMG, L, dtype=F32), vm(c3, IMG, LL, dtype=F32),
        vm(c1, IMG, LL, dtype=F32), vm(c2, IMG, LL, dtype=F32), vm(c3, IMG, LL, dtype=F32),
        vm(c1 + 2, IMG, LL), vm(c2 + 2, IMG, LL), vm(c3 + 2, IMG, LL), vm(c2 + 1, 2, IMG, LL), vm(c3 + 1, 2, IMG, LL),
        vm(2, c3 * IMG, L, dtype=F32),
        *[packed] * 6,
        vm(c1 + 2, IMG, L), vm(c2 + 2, IMG, LL), vm(c3 + 2, IMG, LL), vm(c3 + 2, IMG, LL), vm(c2 + 1, 2, IMG, L), vm(c2 + 1, 2, IMG, L), vm(c3 + 1, 2, IMG, L),
        pltpu.SemaphoreType.DMA((2, 2)), pltpu.SemaphoreType.DMA((5,)), pltpu.SemaphoreType.DMA((SLOTS,)),
        pltpu.SemaphoreType.REGULAR,
    ]

    def local(x_tile, *params):
        x_t = jnp.transpose(x_tile, (0, 1, 3, 2))
        params = [p.reshape(1, -1) if p.ndim == 1 else p for p in params]
        operands = [pltpu.with_memory_space_constraint(p, pltpu.HBM) for p in (x_t, *params)]
        return pl.pallas_call(
            functools.partial(_body, row_count),
            out_shape=pltpu.VMEM((IMG, 1, 32, LL), BF),
            in_specs=[pl.BlockSpec(memory_space=pltpu.HBM)] * len(operands),
            out_specs=pl.BlockSpec(memory_space=pltpu.VMEM),
            scratch_shapes=scratch,
            compiler_params=pltpu.CompilerParams(collective_id=0, has_side_effects=True, vmem_limit_bytes=60 * MIB),
        )(*operands)

    return jax.shard_map(local, mesh=mesh, in_specs=(tile_spec,) + (P(),) * 15, out_specs=tile_spec, check_vma=False)
```

```python
import functools

import jax
import jax.numpy as jnp
from jax import lax
from jax.experimental import pallas as pl
from jax.experimental.pallas import tpu as pltpu
from jax.sharding import PartitionSpec as P

MESH = pl.DeviceIdType.MESH
BF = jnp.bfloat16
F32 = jnp.float32

L = 128
LL = 2 * L
H = L // 2
Q = L // 4
LO = slice(0, L)
HI = slice(L, LL)
IMG = 16
SIZES = (5, 5, 5, 6, 7, 7)
N = len(SIZES)
EDGE = 3
PAD = 12
NEED = (11, 7)
COLS = (140, 70, 35)
STEP = 132
TAPS = range(3)
MIB = 1024 * 1024

(X_TOP, DIAG, X_COL, Y1_DOWN, Y1_UP, Z1_DOWN, Y2_DOWN, Z1_UP, Z2_DOWN, Y3_DOWN, Y3_UP, MESSAGES) = range(12)
SLOT = {X_TOP: (0, 1), DIAG: (2,), X_COL: (3,)}
WEIGHTS = 15
OWN = 4 + WEIGHTS
for i, m in enumerate((Y1_DOWN, Y1_UP, Z1_UP)):
    SLOT[m] = tuple(range(OWN + N * i, OWN + N * i + N))
SLOT[Z2_DOWN], SLOT[Y3_UP] = SLOT[Y1_DOWN], SLOT[Y1_UP]
SLOT[Z1_DOWN], SLOT[Y2_DOWN] = tuple(range(4, 4 + N)), tuple(range(4 + N, 4 + 2 * N))
SLOT[Y3_DOWN] = tuple(range(4 + 2 * N, OWN)) + SLOT[X_TOP] + SLOT[DIAG]
OUT = {X_TOP: 0, DIAG: 1, X_COL: 2, **{m: 3 for m in (Y1_DOWN, Z1_DOWN, Y2_DOWN, Z2_DOWN, Y3_DOWN)},
       **{m: 4 for m in (Y1_UP, Z1_UP, Y3_UP)}}
ROWS_DOWN = 8 * (2 * COLS[1] + COLS[1] - 2 + 2 * (COLS[2] - 1) + 2 * (COLS[2] - 2))
ROWS_UP = 8 * (COLS[1] + 2 * (COLS[1] - 1) + 2 * (COLS[2] - 2))
SLOTS = OWN + 3 * N


def _dot(a, b):
    return jnp.dot(a, b, preferred_element_type=F32)


def _flat(v):
    return v.reshape(v.shape[0] * v.shape[1], v.shape[2])


def _roll(v, shift):
    return pltpu.roll(v, shift, v.ndim - 1)


def _lane(shape):
    return lax.broadcasted_iota(jnp.int32, shape, len(shape) - 1)


def _relu(v):
    return jnp.maximum(v, 0.0)


def _body(row_count, *refs):
    (x_hbm, wd1_h, bd1_h, wc1_h, bc1_h, wp1_h, wd2_h, bd2_h, wc2_h, bc2_h, wp2_h, wd3_h, bd3_h, wc3_h, bc3_h, wp3_h,
     out_ref,
     xv, xt, xtop, xh, fs, sdiag, rdiag, bias,
     wd1r, wc1r, wp1r, wd2r, wc2r, wp2r, wd3, wc3, wp3, bd1, bc1, bd2, bc2, bd3, bc3,
     wd1, wdh1, wc1, wch1, wpp1, wd2, wdh2, wdb2, wc2, wch2, wpp2,
     part1, part2, part3, acc1, acc2, acc3, y1, y2, y3, z1, z2, zo,
     sy1d, sy1u, sz1, ry1d, ry1u, rz1,
     yh1, yh2, yt3, yb3, zh1, zb1, zh2,
     xsem, ssem, rsem, near_sem) = refs

    row = lax.axis_index("row")
    col = lax.axis_index("col")
    outer, inner = col, 1 - col
    has_up = row > 0
    has_down = row < row_count - 1
    up = {"row": row - 1}
    down = {"row": row + 1}
    side = {"col": 1 - col}
    diag_down = {"row": row + 1, "col": 1 - col}

    barrier = pltpu.get_barrier_semaphore()

    def greet(device):
        pl.semaphore_signal(barrier, inc=1, device_id=device, device_id_type=MESH)

    greet(side)

    @pl.when(has_up)
    def _():
        greet(up)

    @pl.when(has_down)
    def _():
        greet(down)

    def x_copy(h, part):
        rows = pl.ds(*((7, 1), (0, 4), (4, 3), (0, 7))[part])
        return pltpu.make_async_copy(x_hbm.at[:, rows, :, pl.ds(pl.multiple_of(h * L, L), L)], xv.at[h, :, rows],
                                     xsem.at[h, min(part, 1)])

    w_copies = [pltpu.make_async_copy(s, d, rsem.at[4 + i]) for i, (s, d) in enumerate(
        ((wd1_h, wd1r), (bd1_h, bd1), (bc1_h, bc1), (bd2_h, bd2), (bc2_h, bc2), (bd3_h, bd3), (bc3_h, bc3),
         (wc1_h, wc1r), (wp1_h, wp1r), (wd2_h, wd2r), (wc2_h, wc2r), (wp2_h, wp2r),
         (wd3_h, wd3), (wc3_h, wc3), (wp3_h, wp3)))]
    first_copies, late_copies = w_copies[:7], w_copies[7:]
    x_copy(outer, 0).start()
    x_copy(inner, 0).start()
    for h in (inner, outer):
        for part in (1, 2):
            x_copy(h, part).start()
    for c in first_copies:
        c.start()

    def span(k, stage):
        before, scale = sum(SIZES[:k]), COLS[stage - 1] // COLS[2]
        first = before + col * (COLS[2] - SIZES[k] - 2 * before)
        return scale * first, scale * SIZES[k]

    def remote(src, dst, msg, k, dev):
        slot = SLOT[msg][k] if isinstance(k, int) else k
        return pltpu.make_async_remote_copy(src_ref=src, dst_ref=dst, send_sem=ssem.at[OUT[msg]], recv_sem=rsem.at[slot],
                                            device_id=dev, device_id_type=MESH)

    def m_xtop(h):
        if h is None:
            return remote(xtop, xtop, X_TOP, 0, down)
        return remote(xv.at[h, :, 7], xtop.at[h], X_TOP, h, down)

    def m_diag():
        return remote(sdiag, rdiag, DIAG, 0, diag_down)

    own_edge = 1 + (L - PAD) * inner + PAD * col
    far_edge = 1 + L * col

    def m_xcol(c):
        skip = (PAD - NEED[0]) * (1 - c)
        return remote(xt.at[pl.ds(own_edge + skip, NEED[c])], xt.at[pl.ds(far_edge + skip, NEED[c])], X_COL, 0, side)

    def for_col(fn):
        for c in range(2):
            @pl.when(col == c)
            def _():
                fn(c)

    def chunk(k, stage, spare):
        first, size = span(k, stage)
        if k == N - 1:
            return pl.ds(1 + first + spare * col, size - spare)
        return pl.ds(1 + first, size)

    def plain(src, dst, msg, dev, stage, spare, src_lanes=None, dst_lanes=None):
        def make(k):
            s = chunk(k, stage, spare)
            return remote(src.at[s] if src_lanes is None else src.at[s, :, src_lanes],
                          dst.at[s] if dst_lanes is None else dst.at[s, :, dst_lanes], msg, k, dev)
        return make

    lanes_lo, lanes_hi = pl.ds(0, L), pl.ds(L, L)
    def packed(src, dst, msg, dev):
        def make(k):
            s = pl.ds(*span(k, 2))
            return remote(src.at[s], dst.at[s], msg, k, dev)
        return make

    m_y1d = packed(sy1d, ry1d, Y1_DOWN, down)
    m_y1u = packed(sy1u, ry1u, Y1_UP, up)
    m_z1 = packed(sz1, rz1, Z1_DOWN, down)
    m_y2d = plain(y2, yh2, Y2_DOWN, down, 2, 2, lanes_hi, lanes_lo)
    m_y3d = plain(y3, yt3, Y3_DOWN, down, 3, 2)
    m_y3u = plain(y3, yb3, Y3_UP, up, 3, 2)

    def m_z1u(k):
        s = chunk(k, 2, 1)
        return remote(z1.at[s, :, :, lanes_lo], zb1.at[s], Z1_UP, k, up)

    def m_z2(k):
        s = chunk(k, 3, 1)
        return remote(z2.at[s, :, :, lanes_hi], zh2.at[s], Z2_DOWN, k, down)

    def send(downs, ups, k):
        if downs:
            @pl.when(has_down)
            def _():
                for m in downs:
                    m(k).start()
        if ups:
            @pl.when(has_up)
            def _():
                for m in ups:
                    m(k).start()

    def recv(downs, ups, k):
        if downs:
            @pl.when(has_up)
            def _():
                for m in downs:
                    m(k).wait_recv()
        if ups:
            @pl.when(has_down)
            def _():
                for m in ups:
                    m(k).wait_recv()

    for ref in (xt, xh, z1, z2, zh1, zb1, zh2, y1, y2, y3, yh1, yh2, yt3, yb3):
        ref[0] = jnp.zeros(ref.shape[1:], BF)
    for ref in (y1, y2, y3, yh1, yh2, yt3, yb3):
        ref[ref.shape[0] - 1] = jnp.zeros(ref.shape[1:], BF)

    vertical = jnp.minimum(row, 1) + jnp.minimum(row_count - 1 - row, 1)
    pl.semaphore_wait(barrier, 1 + vertical)

    for h in (outer, inner):
        x_copy(h, 0).wait()
        send([m_xtop], [], h)
    @pl.when(has_up)
    def _():
        pl.semaphore_signal(near_sem, inc=1, device_id=up, device_id_type=MESH)

    @pl.when(has_down)
    def _():
        pl.semaphore_signal(near_sem, inc=1, device_id=down, device_id_type=MESH)

    for c in late_copies:
        c.start()

    @pl.when(jnp.logical_not(has_up))
    def _():
        for ref in (xtop, rdiag, ry1d, rz1, zh2, yt3):
            ref[...] = jnp.zeros(ref.shape, BF)
        yh2[:, :, LO] = jnp.zeros((yh2.shape[0], IMG, L), BF)

    @pl.when(jnp.logical_not(has_down))
    def _():
        for ref in (ry1u, zb1, yb3):
            ref[...] = jnp.zeros(ref.shape, BF)

    def toeplitz(dst, rows_in, rows_out, shape, piece):
        for r in range(rows_in):
            parts = []
            for i in range(rows_out):
                v = piece(r, i)
                parts.append(jnp.zeros(shape, BF) if v is None else v)
            dst[r * shape[0]:(r + 1) * shape[0], :] = jnp.concatenate(parts, axis=1)

    def tap_of(w, kw, stride):
        def piece(r, i):
            kh = r - stride * i + 1
            return w[kh, kw] if kh in TAPS else None
        return piece

    for c in first_copies:
        c.wait()
    for i, (b, reps) in enumerate(((bd1, 4), (bc1, 4), (bd2, 2), (bc2, 2), (bd3, 1), (bc3, 1))):
        v = jnp.concatenate([b[...]] * reps, axis=-1)
        bias[i] = jnp.broadcast_to(v, (IMG, LL))
    s_d1, s_c1 = wd1r.shape[2:], wc1r.shape[2:]
    for kw in TAPS:
        toeplitz(wd1.at[kw], 8, 4, s_d1, tap_of(wd1r, kw, 2))
    toeplitz(wdh1, 4, 2, s_d1, lambda r, i: wd1r[0, r] if r in TAPS and i == 0 else None)

    def transpose_half(h):
        for n in range(IMG):
            for g in range(2):
                block = xv[h, n, 4 * g:4 * g + 4].reshape(L, L)
                fs[g, n * STEP:n * STEP + L, :] = block.T.astype(F32)

    def gather_pairs(h, lo, n):
        base = 1 + PAD * col + H * h

        @pl.loop(0, n, unroll=4)
        def _(i):
            p = lo + i
            for e in range(2):
                v = [fs[g, pl.ds(2 * p + e, IMG, stride=STEP), :] for g in range(2)]
                xt[base + p, e] = jnp.concatenate(v, axis=-1).astype(BF)

    def transpose_top(h):
        for n in range(IMG):
            block = jnp.concatenate([xtop[h, n]] * 4, axis=0)
            fs[0, n * STEP:n * STEP + L, :] = block.T.astype(F32)
        base = 1 + PAD * col + H * h

        @pl.loop(0, H, unroll=8)
        def _(p):
            for e in range(2):
                xh[base + p, e] = fs[0, pl.ds(2 * p + e, IMG, stride=STEP), :].astype(BF)

    quads = (PAD // 2, 4, IMG, L)

    def pack_diag():
        v = xt[pl.ds(own_edge, PAD), :, :, HI].astype(F32).reshape(quads)
        ln = _lane((quads[0], IMG, L))
        r = v[:, 3]
        for q in TAPS:
            r = jnp.where((ln >= q * Q) & (ln < (q + 1) * Q), _roll(v[:, q], (q + 1) * Q), r)
        sdiag[...] = r.astype(BF)

    def unpack_diag():
        v = rdiag[...].astype(F32)
        ln = _lane(v.shape)
        out = []
        for q in range(4):
            r = jnp.where((ln >= q * Q) & (ln < (q + 1) * Q), v, 0.0)
            r = r + _roll(r, Q)
            out.append(r + _roll(r, H))
        u = jnp.stack(out, axis=1).astype(BF)
        xh[pl.ds(1 + L * (1 - col), PAD)] = u.reshape(PAD, 2, IMG, L)

    border = (H - PAD) * inner
    x_copy(inner, 3).wait()
    transpose_half(inner)
    gather_pairs(inner, border, PAD)
    for_col(lambda c: m_xcol(c).start())
    pack_diag()
    gather_pairs(inner, PAD * col, H - PAD)
    x_copy(outer, 3).wait()
    transpose_half(outer)
    gather_pairs(outer, 0, H)
    pl.semaphore_wait(near_sem, vertical)

    @pl.when(has_down)
    def _():
        m_diag().start()

    def taps(ref, j0, m):
        return [_flat(ref[pl.ds(j0 + t, m)]) for t in TAPS]

    def pair_taps(ref, j0, m):
        return [_flat(ref[pl.ds(j0, m), 1]), _flat(ref[pl.ds(j0 + 1, m), 0]), _flat(ref[pl.ds(j0 + 1, m), 1])]

    def sum_dots(lhs, w):
        v = _dot(lhs[0], w(0))
        for t in TAPS[1:]:
            v = v + _dot(lhs[t], w(t))
        return v

    def sum_narrow(lhs, w):
        pair = jnp.concatenate([w(0), w(1)], axis=0)
        return _dot(jnp.concatenate(lhs[:2], axis=-1), pair) + _dot(lhs[2], w(2))

    def tiles(v, m):
        return v.reshape(m, IMG, v.shape[-1])

    def pack(a, b):
        return jnp.where(_lane(a.shape) < H, a, b).astype(BF)

    def above1(j0, m):
        a, b, c = pair_taps(xh, j0, m)
        ln = _lane(a.shape)
        return tiles(_dot(jnp.where(ln < Q, a, jnp.where(ln < H, b, c)), wdh1[...]), m)

    def store_top1(k, v):
        j0, m = span(k, 1)
        p = m // 2
        lo = _relu(v + bias[0, :, LO])
        y1[pl.ds(1 + j0, m), :, LO] = lo.astype(BF)
        sy1u[pl.ds(*span(k, 2))] = pack(lo[:p], _roll(lo[p:], H))

    def down1(k, whole=False):
        j0, m = span(k, 1)
        p = m // 2
        v = tiles(sum_dots(pair_taps(xt, j0, m), lambda t: wd1[t]), m)
        if whole:
            store_top1(k, v[:, :, LO] + above1(j0, m))
        else:
            part1[pl.ds(j0, m)] = v[:, :, LO]
        hi = _relu(v[:, :, HI] + bias[0, :, HI])
        y1[pl.ds(1 + j0, m), :, HI] = hi.astype(BF)
        sy1d[pl.ds(*span(k, 2))] = pack(_roll(hi[:p], H), hi[p:])

    def top1(k):
        j0, m = span(k, 1)
        store_top1(k, above1(j0, m) + part1[pl.ds(j0, m)])

    def conv1(k):
        j0, m = span(k, 1)
        v = sum_dots(taps(y1, j0, m), lambda t: wc1[t]) + _dot(_flat(xt[pl.ds(j0 + 1, m), 0]), wpp1[...])
        acc1[pl.ds(j0, m)] = tiles(v, m) + bias[1]

    def unpack1(k):
        s, p = span(k, 2)
        j0 = span(k, 1)[0]
        t, b = ry1d[pl.ds(s, p)].astype(F32), ry1u[pl.ds(s, p)].astype(F32)
        yh1[pl.ds(1 + j0, p)] = pack(t, _roll(b, H))
        yh1[pl.ds(1 + j0 + p, p)] = pack(_roll(t, H), b)

    def halo1(k):
        j0, m = span(k, 1)
        s, p = span(k, 2)
        v = tiles(sum_narrow(taps(yh1, j0, m), lambda t: wch1[t]), m)
        v = _relu(v + acc1[pl.ds(j0, m)])
        z1[pl.ds(1 + s, p)] = v.astype(BF).reshape(p, 2, IMG, LL)
        hi = v[:, :, HI]
        sz1[pl.ds(s, p)] = pack(_roll(hi[:p], H), hi[p:])

    def down2(k):
        j0, m2 = span(k, 2)
        v = tiles(sum_dots(pair_taps(z1, j0, m2), lambda t: wd2[t]), m2)
        part2[pl.ds(j0, m2)] = v[:, :, LO]
        y2[pl.ds(1 + j0, m2), :, HI] = _relu(v[:, :, HI] + bias[2, :, HI]).astype(BF)

    def unpack2(k):
        s, p = span(k, 2)
        half = p // 2
        t = rz1[pl.ds(s, p)].astype(F32)
        u = _roll(t, H)
        zh1[pl.ds(1 + s, half)] = pack(t, u).reshape(half, 2, IMG, L)
        zh1[pl.ds(1 + s + half, half)] = pack(u, t).reshape(half, 2, IMG, L)

    def top2(k):
        j0, m2 = span(k, 2)
        a, b, c = pair_taps(zh1, j0, m2)
        t = jnp.concatenate([jnp.where(_lane(a.shape) < H, a, b), c], axis=-1)
        v = tiles(_dot(t, wdh2[...]), m2) + part2[pl.ds(j0, m2)]
        y2[pl.ds(1 + j0, m2), :, LO] = _relu(v + bias[2, :, LO]).astype(BF)

    def bottom2(k):
        j0, m2 = span(k, 2)
        own, below = pair_taps(z1, j0, m2), pair_taps(zb1, j0, m2)
        lhs = [jnp.concatenate([a[:, HI], b], axis=-1) for a, b in zip(own, below)]
        v = _relu(tiles(sum_dots(lhs, lambda t: wdb2[t]), m2) + bias[2, :, LO])
        yh2[pl.ds(1 + j0, m2), :, HI] = jnp.where(has_down, v, 0.0).astype(BF)

    def conv2(k):
        j0, m2 = span(k, 2)
        v = sum_dots(taps(y2, j0, m2), lambda t: wc2[t]) + _dot(_flat(z1[pl.ds(j0 + 1, m2), 0]), wpp2[...])
        acc2[pl.ds(j0, m2)] = tiles(v, m2) + bias[3]

    def halo2(k):
        j0, m2 = span(k, 2)
        v = tiles(sum_dots(taps(yh2, j0, m2), lambda t: wch2[t]), m2) + acc2[pl.ds(j0, m2)]
        s, p = span(k, 3)
        z2[pl.ds(1 + s, p)] = _relu(v).astype(BF).reshape(p, 2, IMG, LL)

    def down3(k):
        j0, m3 = span(k, 3)
        v = sum_dots(pair_taps(z2, j0, m3), lambda t: wd3[1:, t].reshape(LL, LL))
        part3[pl.ds(j0, m3)] = tiles(v, m3) + bias[4]

    def top3(k):
        j0, m3 = span(k, 3)
        v = tiles(sum_narrow(pair_taps(zh2, j0, m3), lambda t: wd3[0, t]), m3) + part3[pl.ds(j0, m3)]
        y3[pl.ds(1 + j0, m3)] = _relu(v).astype(BF)

    def conv3(k):
        j0, m3 = span(k, 3)
        v = sum_dots(taps(y3, j0, m3), lambda t: wc3[1, t]) + _dot(_flat(z2[pl.ds(j0 + 1, m3), 0, :, LO]), wp3[...])
        acc3[pl.ds(j0, m3)] = tiles(v, m3) + bias[5]

    def add3(k, rows, kh):
        j0, m3 = span(k, 3)
        s = pl.ds(j0, m3)
        acc3[s] = acc3[s] + tiles(sum_dots(taps(rows, j0, m3), lambda t: wc3[kh, t]), m3)

    def halo3(k, rows, kh):
        j0, m3 = span(k, 3)
        v = tiles(sum_dots(taps(rows, j0, m3), lambda t: wc3[kh, t]), m3)
        v = _relu(v + acc3[pl.ds(j0, m3)])
        r = pl.ds(pl.multiple_of(j0 * IMG, IMG), m3 * IMG)
        zo[0, r] = _flat(v[:, :, LO])
        zo[1, r] = _flat(v[:, :, HI])

    last = N - 1

    def wait_next(downs, ups, k):
        if k == 0:
            recv(downs, ups, 0)
        if k < last:
            recv(downs, ups, k + 1)

    for k in range(last):
        down1(k)
    for k in range(last):
        send([m_y1d], [], k)

    for c in late_copies:
        c.wait()
    for kw in TAPS:
        toeplitz(wc1.at[kw], 4, 4, s_c1, tap_of(wc1r, kw, 1))
        toeplitz(wch1.at[kw], 2, 4, s_c1, lambda r, i: wc1r[2 * r, kw] if i == 3 * r else None)
    toeplitz(wpp1, 8, 4, s_d1, lambda r, i: wp1r[...] if r == 2 * i else None)

    s_d2, s_c2 = wd2r.shape[2:], wc2r.shape[2:]
    for kw in TAPS:
        toeplitz(wd2.at[kw], 4, 2, s_d2, tap_of(wd2r, kw, 2))
        toeplitz(wdb2.at[kw], 4, 1, s_d2, lambda r, i: wd2r[r - 1, kw] if r else None)
        toeplitz(wc2.at[kw], 2, 2, s_c2, tap_of(wc2r, kw, 1))
        toeplitz(wch2.at[kw], 2, 2, s_c2, lambda r, i: wc2r[2 * r, kw] if i == r else None)
    toeplitz(wpp2, 4, 2, s_d2, lambda r, i: wp2r[...] if r == 2 * i else None)
    toeplitz(wdh2, 4, 1, s_d2, lambda r, i: wd2r[0, r] if r in TAPS else None)

    recv([m_xtop], [], outer)
    transpose_top(outer)
    for k in range(EDGE):
        top1(k)
        send([], [m_y1u], k)

    recv([m_xtop], [], inner)
    transpose_top(inner)
    for k in range(EDGE, last):
        top1(k)
    for k in range(EDGE, last):
        send([], [m_y1u], k)
    conv1(0)

    def border1():
        @pl.when(has_up)
        def _():
            m_diag().wait_recv()

        for_col(lambda c: m_xcol(1 - c).wait_recv())
        unpack_diag()
        down1(last, True)
        send([m_y1d], [m_y1u], last)

    def first_z1():
        for k in range(2):
            recv([m_y1d], [m_y1u], k)
            unpack1(k)
        halo1(0)
        conv1(1)
        send([m_z1], [m_z1u], 0)

    border1()
    first_z1()

    for k in range(1, N):
        if k < last:
            recv([m_y1d], [m_y1u], k + 1)
            unpack1(k + 1)
        if k >= 2:
            down2(k - 2)
        halo1(k)
        if k < last:
            conv1(k + 1)
        send([m_z1], [m_z1u], k)
    for k in range(N - 2):
        send([m_y2d], [], k)
    down2(last - 1)
    down2(last)
    send([m_y2d], [], last - 1)
    send([m_y2d], [], last)

    def above2(k):
        if k == 0:
            recv([m_z1], [], 0)
            unpack2(0)
        if k < last:
            recv([m_z1], [], k + 1)
            unpack2(k + 1)
        if k >= 2:
            conv2(k - 2)
        top2(k)

    def recv_left(m, k):
        if k == 0:
            recv([m], [], 0)
        else:
            @pl.when(jnp.logical_and(has_up, col == 0))
            def _():
                m(k).wait_recv()
        if k < last:
            @pl.when(jnp.logical_and(has_up, col == 1))
            def _():
                m(k + 1).wait_recv()

    above2(0)
    above2(1)
    recv([], [m_z1u], 0)
    for k in range(last):
        if k + 2 < N:
            above2(k + 2)
        else:
            conv2(last - 1)
            conv2(last)
        if k == last - 1:
            recv_left(m_z2, 0)
            top3(0)
            send([m_y3d], [m_y3u], 0)
        recv([], [m_z1u], k + 1)
        bottom2(k)
        if k == last - 1:
            bottom2(last)
        if k:
            wait_next([m_y2d], [], k - 1)
            if k >= 3:
                down3(k - 3)
            halo2(k - 1)
            send([m_z2], [], k - 1)
    recv([m_y2d], [], last)
    down3(last - 3)
    halo2(last - 1)
    halo2(last)
    send([m_z2], [], last - 1)
    send([m_z2], [], last)

    for k in range(1, N):
        recv_left(m_z2, k)
        top3(k)
        if k < 4:
            down3(last - 3 + k)
        send([m_y3d], [m_y3u], k)
    for k in range(N):
        conv3(k)

    half = IMG

    def write_out(h):
        lo = pl.multiple_of(half * h, half)
        for n in range(IMG):
            v = [zo[g, pl.ds(PAD * 4 * col + half * IMG * h + n, half, stride=IMG), :] for g in range(2)]
            out_ref[n, 0, pl.ds(lo, half)] = jnp.concatenate(v, axis=-1).astype(BF)

    for_col(lambda c: m_xcol(c).wait_send())

    @pl.when(has_down)
    def _():
        m_diag().wait_send()
        m_xtop(None).wait_send()

    def all_sent(msg, rows, dev):
        ref = fs.at[:, pl.ds(0, rows // 2)]
        remote(ref, ref, msg, 0, dev).wait_send()

    def finish(near, far):
        near_recv, near_rows, near_kh = near
        far_recv, far_rows, far_kh = far
        for k in range(N):
            near_recv(k)
        for k in range(N):
            add3(k, near_rows, near_kh)
        far_recv(0)
        for k in range(last - 1):
            far_recv(k + 1)
            halo3(k, far_rows, far_kh)
        write_out(outer)
        far_recv(last)
        halo3(last - 1, far_rows, far_kh)
        halo3(last, far_rows, far_kh)
        write_out(inner)

    above = (lambda k: recv([m_y3d], [], k), yt3, 0)
    below = (lambda k: recv([], [m_y3u], k), yb3, 2)
    near_below = lax.rem(row, 2) == 0

    @pl.when(near_below)
    def _():
        finish(below, above)

    @pl.when(jnp.logical_not(near_below))
    def _():
        finish(above, below)

    @pl.when(has_down)
    def _():
        all_sent(Y1_DOWN, ROWS_DOWN, down)

    @pl.when(has_up)
    def _():
        all_sent(Y1_UP, ROWS_UP, up)


def solution(mesh):
    row_count = mesh.shape["row"]
    tile_spec = P("batch", "row", "col")
    c1, c2, c3 = COLS

    def vm(*shape, dtype=BF):
        return pltpu.VMEM(shape, dtype)

    def weights(cin, cout):
        return [vm(3, 3, cin, cout), vm(3, 3, cout, cout), vm(cin, cout)]

    packed = vm(c2, IMG, L)
    scratch = [
        vm(2, IMG, 8, Q, L), vm(c1 + 1, 2, IMG, LL), vm(2, IMG, Q, L), vm(c1 + 1, 2, IMG, L),
        vm(2, IMG * STEP, L, dtype=F32), vm(PAD // 2, IMG, L), vm(PAD // 2, IMG, L), vm(6, IMG, LL, dtype=F32),
        *weights(Q, H), *weights(H, L), *weights(L, LL),
        *[vm(1, c, dtype=F32) for c in (H, H, L, L, LL, LL)],
        vm(3, LL, LL), vm(L, L), vm(3, LL, LL), vm(3, L, LL), vm(LL, LL),
        vm(3, LL, LL), vm(LL, L), vm(3, LL, L), vm(3, LL, LL), vm(3, LL, LL), vm(LL, LL),
        vm(c1, IMG, L, dtype=F32), vm(c2, IMG, L, dtype=F32), vm(c3, IMG, LL, dtype=F32),
        vm(c1, IMG, LL, dtype=F32), vm(c2, IMG, LL, dtype=F32), vm(c3, IMG, LL, dtype=F32),
        vm(c1 + 2, IMG, LL), vm(c2 + 2, IMG, LL), vm(c3 + 2, IMG, LL), vm(c2 + 1, 2, IMG, LL), vm(c3 + 1, 2, IMG, LL),
        vm(2, c3 * IMG, L, dtype=F32),
        *[packed] * 6,
        vm(c1 + 2, IMG, L), vm(c2 + 2, IMG, LL), vm(c3 + 2, IMG, LL), vm(c3 + 2, IMG, LL), vm(c2 + 1, 2, IMG, L), vm(c2 + 1, 2, IMG, L), vm(c3 + 1, 2, IMG, L),
        pltpu.SemaphoreType.DMA((2, 2)), pltpu.SemaphoreType.DMA((5,)), pltpu.SemaphoreType.DMA((SLOTS,)),
        pltpu.SemaphoreType.REGULAR,
    ]

    def local(x_tile, *params):
        x_t = jnp.transpose(x_tile, (0, 1, 3, 2))
        params = [p.reshape(1, -1) if p.ndim == 1 else p for p in params]
        operands = [pltpu.with_memory_space_constraint(p, pltpu.HBM) for p in (x_t, *params)]
        return pl.pallas_call(
            functools.partial(_body, row_count),
            out_shape=pltpu.VMEM((IMG, 1, 32, LL), BF),
            in_specs=[pl.BlockSpec(memory_space=pltpu.HBM)] * len(operands),
            out_specs=pl.BlockSpec(memory_space=pltpu.VMEM),
            scratch_shapes=scratch,
            compiler_params=pltpu.CompilerParams(collective_id=0, has_side_effects=True, vmem_limit_bytes=60 * MIB),
        )(*operands)

    return jax.shard_map(local, mesh=mesh, in_specs=(tile_spec,) + (P(),) * 15, out_specs=tile_spec, check_vma=False)
```
